256 devices in a mesh: gx: 4 (over y_lo, core), gz: 8 (over y_hi, x), ta: 8 (over z).
Axes of the slice: x: 4, y: 4 (y_hi: 2, y_lo: 2; y = y_hi * 2 + y_lo), z: 8, core: 2. Of those that a mesh axis runs over, the one named last changes fastest.
Arguments:
- links: float32 [4, 2, 3, 3, 32, 32, 512], P(None, None, None, None, 'ta', 'gz', 'gx'), may hold values from -1 to 1, as said below
Outputs:
- force: float32 [4, 2, 3, 3, 32, 32, 512], P(None, None, None, None, 'ta', 'gz', 'gx')
The draws below stay inside these ranges and needn't reach their ends.
Inputs may be any that keep to these rules, and one draw needn't show every extreme that they name: Every link matrix (real part links[mu, 0], imaginary part links[mu, 1]) is special unitary, up to float32 rounding.
All inputs are finite; a program needn't handle non-finite values.
Results may differ from the reference program's by a relative error of at most 0.0003.
Values sent between devices are 32-bit elements; how exact they have to be, the bound alone decides.
A program may use at most 64 MiB of HBM per device.

```python
import jax
import jax.numpy as jnp

NX = 16
NY = 32
NZ = 32
NT = 32
NXY = 512


def draw_links(key, part):
    sample = jax.random.normal(key, (2, 4, 3, 3, NT, NZ, NXY), jnp.float32)
    real0 = sample[0][:, 0]
    imag0 = sample[1][:, 0]
    length0 = jnp.maximum(jnp.sqrt(jnp.sum(real0 * real0 + imag0 * imag0, axis=1, keepdims=True)), 1e-06)
    real0 = real0 / length0
    imag0 = imag0 / length0
    real1 = sample[0][:, 1]
    imag1 = sample[1][:, 1]
    inner_real = jnp.sum(real0 * real1 + imag0 * imag1, axis=1, keepdims=True)
    inner_imag = jnp.sum(real0 * imag1 - imag0 * real1, axis=1, keepdims=True)
    real1 = real1 - (inner_real * real0 - inner_imag * imag0)
    imag1 = imag1 - (inner_real * imag0 + inner_imag * real0)
    length1 = jnp.maximum(jnp.sqrt(jnp.sum(real1 * real1 + imag1 * imag1, axis=1, keepdims=True)), 1e-06)
    real1 = real1 / length1
    imag1 = imag1 / length1
    real_cols = []
    imag_cols = []
    for column in range(3):
        next_col = (column + 1) % 3
        last_col = (column + 2) % 3
        cross_real = real0[:, next_col] * real1[:, last_col] - imag0[:, next_col] * imag1[:, last_col] - real0[:, last_col] * real1[:, next_col] + imag0[:, last_col] * imag1[:, next_col]
        cross_imag = real0[:, next_col] * imag1[:, last_col] + imag0[:, next_col] * real1[:, last_col] - real0[:, last_col] * imag1[:, next_col] - imag0[:, last_col] * real1[:, next_col]
        real_cols.append(cross_real)
        imag_cols.append(-cross_imag)
    real2 = jnp.stack(real_cols, axis=1)
    imag2 = jnp.stack(imag_cols, axis=1)
    real_rows = jnp.stack([real0, real1, real2], axis=1)
    imag_rows = jnp.stack([imag0, imag1, imag2], axis=1)
    return jnp.stack([real_rows, imag_rows], axis=1)


def setup_inputs(seed: int = 0) -> dict:
    seeds = jax.random.split(jax.random.key(seed), 2)
    links = draw_links(jax.random.fold_in(seeds[1], 71), 0)
    return dict(links=links)


COEFF = -1.9


def matprod(left, right):
    total = left[:, 0][:, None] * right[0][None, :]
    total = total + left[:, 1][:, None] * right[1][None, :]
    return total + left[:, 2][:, None] * right[2][None, :]


def complex_mul(left, right):
    return (matprod(left[0], right[0]) - matprod(left[1], right[1]),
            matprod(left[0], right[1]) + matprod(left[1], right[0]))


def dagger(matrix):
    return (jnp.swapaxes(matrix[0], 0, 1), -jnp.swapaxes(matrix[1], 0, 1))


def unit_step(direction, sign):
    offset = [0, 0, 0, 0]
    offset[direction] = sign
    return tuple(offset)


def joined(first_step, second_step):
    return tuple(first_step[position] + second_step[position] for position in range(4))


def gauge_force(fetch_link):
    blocks = []
    still = (0, 0, 0, 0)
    for direction in range(4):
        ahead = unit_step(direction, 1)
        summed = None
        for transverse in range(4):
            if transverse == direction:
                continue
            side_up = unit_step(transverse, 1)
            side_down = unit_step(transverse, -1)
            upper = complex_mul(complex_mul(fetch_link(transverse, ahead), dagger(fetch_link(direction, side_up))),
                                dagger(fetch_link(transverse, still)))
            lower = complex_mul(complex_mul(dagger(fetch_link(transverse, joined(ahead, side_down))),
                                            dagger(fetch_link(direction, side_down))),
                                fetch_link(transverse, side_down))
            staple = (upper[0] + lower[0], upper[1] + lower[1])
            summed = staple if summed is None else (summed[0] + staple[0], summed[1] + staple[1])
        loop_matrix = complex_mul(fetch_link(direction, still), summed)
        real_part = 0.5 * (loop_matrix[0] - jnp.swapaxes(loop_matrix[0], 0, 1))
        imag_part = 0.5 * (loop_matrix[1] + jnp.swapaxes(loop_matrix[1], 0, 1))
        trace_third = (loop_matrix[1][0, 0] + loop_matrix[1][1, 1] + loop_matrix[1][2, 2]) / 3.0
        identity = jnp.eye(3, dtype=jnp.float32).reshape((3, 3) + (1,) * trace_third.ndim)
        imag_part = imag_part - identity * trace_third
        blocks.append(COEFF * jnp.stack([real_part, imag_part], axis=0))
    return jnp.stack(blocks, axis=0)


def reference(links):
    lattice = links.reshape(links.shape[:6] + (NY, NX))

    def fetch_link(direction, offset):
        field = lattice[direction]
        field = jnp.roll(field, (-offset[0], -offset[1], -offset[2], -offset[3]), axis=(3, 4, 5, 6))
        return (field[0], field[1])

    return gauge_force(fetch_link).reshape(links.shape)
```

```python
import jax
import jax.numpy as jnp
from jax import lax
from jax.experimental import pallas as pl
from jax.experimental.pallas import tpu as pltpu
from jax.sharding import PartitionSpec as P

COEFF = -1.9
MESH = pl.DeviceIdType.MESH
AXES = ("ta", "gz", "gx")
ROWS2 = 12
FULL = 18
CORNERS = ((0, 1), (0, 2), (1, 0), (1, 2), (2, 0), (2, 1))


def rs(v, k):
    k = k % 8
    return v if k == 0 else pltpu.roll(v, k, axis=0)


def rl(v, k):
    k = k % 128
    return v if k == 0 else pltpu.roll(v, k, axis=1)


def sublane():
    return lax.broadcasted_iota(jnp.int32, (8, 128), 0)


def lanes():
    return lax.broadcasted_iota(jnp.int32, (8, 128), 1)


def total(terms):
    out = terms[0]
    for t in terms[1:]:
        out = out + t
    return out


def mul_nn(a, b):
    return [
        [
            (
                total([a[i][k][0] * b[k][j][0] for k in range(3)])
                - total([a[i][k][1] * b[k][j][1] for k in range(3)]),
                total([a[i][k][0] * b[k][j][1] for k in range(3)])
                + total([a[i][k][1] * b[k][j][0] for k in range(3)]),
            )
            for j in range(3)
        ]
        for i in range(3)
    ]


def mul_hn(a, b):
    return [
        [
            (
                total([a[k][i][0] * b[k][j][0] for k in range(3)])
                + total([a[k][i][1] * b[k][j][1] for k in range(3)]),
                total([a[k][i][0] * b[k][j][1] for k in range(3)])
                - total([a[k][i][1] * b[k][j][0] for k in range(3)]),
            )
            for j in range(3)
        ]
        for i in range(3)
    ]


def mul_nh(a, b):
    return [
        [
            (
                total([a[i][k][0] * b[j][k][0] for k in range(3)])
                + total([a[i][k][1] * b[j][k][1] for k in range(3)]),
                total([a[i][k][1] * b[j][k][0] for k in range(3)])
                - total([a[i][k][0] * b[j][k][1] for k in range(3)]),
            )
            for j in range(3)
        ]
        for i in range(3)
    ]


def third_row(m):
    row = []
    for col in range(3):
        n, q = (col + 1) % 3, (col + 2) % 3
        r0n, i0n = m[0][n]
        r0q, i0q = m[0][q]
        r1n, i1n = m[1][n]
        r1q, i1q = m[1][q]
        row.append(
            (
                (r0n * r1q - i0n * i1q) - (r0q * r1n - i0q * i1n),
                (r0q * i1n + i0q * r1n) - (r0n * i1q + i0n * r1q),
            )
        )
    return row


def gather(entry, rows=3):
    return [[(entry(i * 6 + j), entry(i * 6 + 3 + j)) for j in range(3)] for i in range(rows)]


def scatter(put, m, first=0):
    for i, row in enumerate(m):
        for j, (re, im) in enumerate(row):
            put((first + i) * 6 + j, re)
            put((first + i) * 6 + 3 + j, im)


def kernel(
    x_hbm, o_hbm, u, v, p, l, s, a, o,
    sft, sbt, sfz, sbz, sfy, sby, sc,
    hft, hbt, hfz, hbz, hfy, hby, hc, lt, lz, ly,
    in_sem, out_sem, send_sem, recv_sem,
):
    me = {axis: lax.axis_index(axis) for axis in AXES}
    size = {axis: lax.axis_size(axis) for axis in AXES}

    def at(steps):
        return {
            AXES[d]: lax.rem(me[AXES[d]] + (step + size[AXES[d]]), size[AXES[d]])
            for d, step in steps
        }

    barrier = pltpu.get_barrier_semaphore()
    targets = [at(((d, sgn),)) for d in range(3) for sgn in (-1, 1)]
    targets += [at(((back, 1), (ahead, -1))) for back, ahead in CORNERS]
    for target in targets:
        pl.semaphore_signal(barrier, inc=1, device_id=target, device_id_type=MESH)

    loads = [pltpu.make_async_copy(x_hbm.at[d], u.at[d], in_sem.at[d]) for d in range(4)]
    for load in loads:
        load.start()
    for load in loads:
        load.wait()

    def link(d, c, h):
        return u[d, (c // 3) % 2, c // 6, c % 3, h]

    def slink(d, c, h):
        return u[d, lax.rem(lax.div(c, 3), 2), lax.div(c, 6), lax.rem(c, 3), h]

    sub, lane = sublane(), lanes()
    low = sub < 4
    zrow = lax.rem(sub, 4)
    group = lax.div(lane, 16)
    xcol = lax.rem(lane, 16)

    for c in range(ROWS2):
        for pair in range(2):
            sft[c, pair] = jnp.where(low, link(2 * pair, c, 0), rs(link(2 * pair + 1, c, 0), 4))
            sbt[c, pair] = jnp.where(low, rs(link(2 * pair, c, 1), 4), link(2 * pair + 1, c, 1))
        for h in range(2):
            first, last = link(0, c, h), rs(link(0, c, h), -3)
            for k in range(1, 4):
                first = jnp.where(zrow == k, rs(link(k, c, h), k), first)
                last = jnp.where(zrow == k, rs(link(k, c, h), k - 3), last)
            sfz[c, h] = first
            sbz[c, h] = last
        first, last = link(0, c, 0), rl(link(0, c, 0), -112)
        for g in range(1, 8):
            first = jnp.where(group == g, rl(link(g % 4, c, g // 4), 16 * g), first)
            last = jnp.where(group == g, rl(link(g % 4, c, g // 4), 16 * (g - 7)), last)
        sfy[c] = first
        sby[c] = last

    def merged(items):
        out = items[0][1]
        for mask, value in items[1:]:
            out = jnp.where(mask, value, out)
        return out

    for w in range(2):
        six = range(6)
        sc[0, w] = merged([(sub == r, rs(link(0, w * 6 + r, 1), r - 4)) for r in six])
        sc[1, w] = merged([(group == g, rl(link(0, w * 6 + g, 1), 16 * g)) for g in six])
        sc[2, w] = merged([(sub == r, rs(link(1, w * 6 + r, 0), r - 3)) for r in six])
        sc[3, w] = merged(
            [
                ((group == g) & (zrow == t), rl(rs(link(1, t * 6 + g, w), t - 3), 16 * g))
                for t in range(2)
                for g in six
            ]
        )
        sc[4, w] = merged([(group == g, rl(link(2, w * 6 + g, 0), 16 * (g - 7))) for g in six])
        sc[5, w] = merged(
            [
                ((group == g) & (zrow == t), rl(rs(link(2, t * 6 + g, w), t), 16 * (g - 7)))
                for t in range(2)
                for g in six
            ]
        )

    def send(n, src, dst, target):
        return pltpu.make_async_remote_copy(
            src_ref=src,
            dst_ref=dst,
            send_sem=send_sem.at[n],
            recv_sem=recv_sem.at[n],
            device_id=target,
            device_id_type=MESH,
        )

    two = pl.ds(0, ROWS2)
    corner = [
        send(6 + n, sc.at[n], hc.at[n], at(((back, 1), (ahead, -1))))
        for n, (back, ahead) in enumerate(CORNERS)
    ]
    ahead_faces = [
        send(0, sft, hft.at[two], at(((0, -1),))),
        send(1, sfz, hfz.at[two], at(((1, -1),))),
        send(2, sfy, hfy.at[two], at(((2, -1),))),
    ]
    back_faces = [
        send(3, sbt, hbt.at[two], at(((0, 1),))),
        send(4, sbz, hbz.at[two], at(((1, 1),))),
        send(5, sby, hby.at[two], at(((2, 1),))),
    ]
    pl.semaphore_wait(barrier, len(targets))
    for copy in ahead_faces + back_faces + corner:
        copy.start()

    def ahead_x(field):
        return jnp.where(xcol == 15, rl(field, 15), rl(field, -1))

    def products(n, carry):
        pair, h = lax.div(n, 2), lax.rem(n, 2)
        mu = lax.div(pair, 3)
        nu = lax.rem(mu + 1 + lax.rem(pair, 3), 4)
        own = gather(lambda c: link(mu, c, h))
        far = gather(lambda c: v[pair, c, h])
        prod = mul_nn(own, far)

        def put_p(c, value):
            p[pair, c, h] = value

        def put_l(c, value):
            l[pair, c, h] = value

        scatter(put_p, prod)
        scatter(put_l, mul_hn(prod, gather(lambda c: link(nu, c, h))))
        return carry

    def shift_x(c, carry):
        for j in range(3):
            for h in range(2):
                v[9 + j, c, h] = ahead_x(slink(j, c, h))
        return carry

    lax.fori_loop(0, FULL, shift_x, 0)
    lax.fori_loop(18, 24, products, 0)

    for copy in ahead_faces:
        copy.wait_recv()

    def complete(ref, index):
        m = gather(lambda c: ref[(c,) + index], 2)

        def put(c, value):
            ref[(c,) + index] = value

        scatter(put, [third_row(m)], 2)

    for n in range(2):
        complete(hft, (n,))
        complete(hfz, (n,))
    complete(hfy, ())

    def shift_ahead(c, carry):
        for j in range(3):
            nu = 1 + j
            v0, v1 = slink(nu, c, 0), slink(nu, c, 1)
            r0, r1 = rs(v0, 4), rs(v1, 4)
            halo = hft[c, nu // 2]
            halo = halo if nu % 2 else rs(halo, 4)
            v[j, c, 0] = jnp.where(low, r0, r1)
            v[j, c, 1] = jnp.where(low, r1, halo)
        for j in range(3):
            nu = (2 + j) % 4
            for h in range(2):
                v[3 + j, c, h] = jnp.where(
                    zrow == 3, rs(hfz[c, h], 3 - nu), rs(slink(nu, c, h), -1)
                )
        halo = hfy[c]
        for j in range(3):
            nu = (3 + j) % 4
            for h in range(2):
                v[6 + j, c, h] = jnp.where(
                    group == 7, rl(halo, 16 * (7 - h * 4 - nu)), rl(slink(nu, c, h), -16)
                )
        return carry

    lax.fori_loop(0, FULL, shift_ahead, 0)
    lax.fori_loop(0, 18, products, 0)

    def plaquettes(n, carry):
        index, h = lax.div(n, 2), lax.rem(n, 2)
        far = lax.div(index, 4)
        mu = lax.rem(index, 4)
        nu = lax.rem(mu + 1 + far, 4)
        q = mul_nh(
            gather(lambda c: p[mu * 3 + far, c, h]), gather(lambda c: p[nu * 3 + 2 - far, c, h])
        )
        n = 0
        for i in range(3):
            a[index, n, h] = q[i][i][1] + q[i][i][1]
            n += 1
        for i in range(3):
            for j in range(i + 1, 3):
                a[index, n, h] = q[i][j][0] - q[j][i][0]
                a[index, n + 1, h] = q[i][j][1] + q[j][i][1]
                n += 2
        return carry

    lax.fori_loop(0, 12, plaquettes, 0)

    for copy in back_faces + corner:
        copy.wait_recv()
    for n in range(2):
        complete(hbt, (n,))
        complete(hbz, (n,))
    complete(hby, ())

    def face(ref, index, own, far12, out):
        far = gather(far12, 2)
        far = far + [third_row(far)]
        prod = mul_nn(gather(lambda c: ref[(c,) + index]), far)

        def put(c, value):
            out[(c,) + index] = value

        scatter(put, mul_hn(prod, gather(own)))

    def own_t(c):
        field = hbt[c, 0]
        return jnp.where(low, field, rs(field, 4))

    def far_t0(c):
        return jnp.where(sub == 7, rs(hc[0, c // 6], 7 - c % 6), rs(hbt[c, 0], 3))

    def far_t1(c):
        field = hbt[c, 0]
        edge = rl(rs(hc[1, c // 6], 4), 16 * (7 - c % 6))
        return jnp.where(
            low, jnp.where(group == 7, edge, rl(field, -16)), ahead_x(rs(field, 4))
        )

    face(hbt, (0,), own_t, far_t0, lt)
    face(hbt, (1,), own_t, far_t1, lt)

    for h in range(2):

        def own_z(c):
            field = hbz[c, h]
            return jnp.where(
                zrow == 0,
                rs(field, -1),
                jnp.where(zrow == 2, rs(field, 1), jnp.where(zrow == 3, rs(field, 2), field)),
            )

        def far_z(c):
            if h == 0:
                step_t = jnp.where(low, rs(hbz[c, 0], 3), rs(hbz[c, 1], 3))
            else:
                step_t = jnp.where(low, rs(hbz[c, 1], 3), rs(hc[2, c // 6], 4 - c % 6))
            field = hbz[c, h]
            edge = rl(rs(hc[3, h], 2 - c // 6), 16 * (7 - c % 6))
            step_y = jnp.where(group == 7, edge, rl(rs(field, 1), -16))
            step_x = ahead_x(rs(field, 2))
            return jnp.where(zrow == 0, step_t, jnp.where(zrow == 3, step_x, step_y))

        face(hbz, (h,), own_z, far_z, lz)

    def own_y(c):
        field = hby[c]
        slot = lax.rem(group, 4)
        return jnp.where(
            slot == 0,
            rl(field, -32),
            jnp.where(slot == 1, rl(field, -16), jnp.where(slot == 3, rl(field, 16), field)),
        )

    def far_y(c):
        field = hby[c]
        slot = lax.rem(group, 4)
        turned = rs(field, 4)
        edge = rs(rl(hc[4, c // 6], 16 * (4 - c % 6)), 4)
        high = jnp.where(group == 4, edge, rl(turned, 32))
        step_t = jnp.where(low, rl(turned, -32), high)
        edge0 = rs(rl(hc[5, 0], 16 * (1 - c % 6)), 3 - c // 6)
        edge1 = rs(rl(hc[5, 1], 16 * (5 - c % 6)), 3 - c // 6)
        step_z = jnp.where(
            zrow == 3, jnp.where(group == 1, edge0, edge1), rl(rs(field, -1), -16)
        )
        step_x = rl(ahead_x(field), 16)
        return jnp.where(slot == 0, step_t, jnp.where(slot == 3, step_x, step_z))

    face(hby, (), own_y, far_y, ly)

    def shift_back(c, carry):
        for h in range(2):
            for mu in range(4):
                terms = []
                for j in range(3):
                    nu = (mu + 1 + j) % 4
                    field = l[mu * 3 + j, c, h]
                    if nu == 0:
                        turned = rs(l[mu * 3 + j, c, 0], 4)
                        if h == 0:
                            halo = lt[c, mu // 2]
                            moved = jnp.where(low, rs(halo, 4) if mu % 2 else halo, turned)
                        else:
                            moved = jnp.where(low, turned, rs(field, 4))
                    elif nu == 1:
                        moved = jnp.where(zrow == 0, rs(lz[c, h], -mu), rs(field, 1))
                    elif nu == 2:
                        moved = jnp.where(
                            group == 0, rl(ly[c], -16 * (h * 4 + mu)), rl(field, 16)
                        )
                    else:
                        moved = jnp.where(xcol == 0, rl(field, -15), rl(field, 1))
                    terms.append(moved)
                s[mu, c, h] = total(terms)
        return carry

    lax.fori_loop(0, FULL, shift_back, 0)

    def forces(n, carry):
        mu, h = lax.div(n, 2), lax.rem(n, 2)
        w = mul_nn(gather(lambda c: link(mu, c, h)), gather(lambda c: s[mu, c, h]))
        prev = lax.rem(mu + 3, 4)
        pick = 4 + lax.rem(mu, 2)
        sign = 1.0 - 2.0 * lax.div(mu, 2).astype(jnp.float32)

        def extra(k):
            return a[mu, k, h] - a[prev, k, h] + sign * a[pick, k, h]

        diag = [w[i][i][1] + w[i][i][1] + extra(i) for i in range(3)]
        third = total(diag) * (1.0 / 3.0)
        for i in range(3):
            o[mu, 0, i, i, h] = jnp.zeros((8, 128), jnp.float32)
            o[mu, 1, i, i, h] = (0.5 * COEFF) * (diag[i] - third)
        k = 3
        for i in range(3):
            for j in range(i + 1, 3):
                re = (0.5 * COEFF) * (w[i][j][0] - w[j][i][0] + extra(k))
                im = (0.5 * COEFF) * (w[i][j][1] + w[j][i][1] + extra(k + 1))
                o[mu, 0, i, j, h] = re
                o[mu, 0, j, i, h] = -re
                o[mu, 1, i, j, h] = im
                o[mu, 1, j, i, h] = im
                k += 2
        return carry

    stores = [pltpu.make_async_copy(o.at[d], o_hbm.at[d], out_sem.at[d]) for d in range(4)]
    for d in range(4):
        lax.fori_loop(2 * d, 2 * d + 2, forces, 0)
        stores[d].start()
    for copy in ahead_faces + back_faces + corner:
        copy.wait_send()
    for store in stores:
        store.wait()


def per_device(links):
    shape = (4, 2, 3, 3, 2, 8, 128)
    f32 = jnp.float32
    out = pl.pallas_call(
        kernel,
        out_shape=jax.ShapeDtypeStruct(shape, f32),
        in_specs=[pl.BlockSpec(memory_space=pltpu.HBM)],
        out_specs=pl.BlockSpec(memory_space=pltpu.HBM),
        scratch_shapes=[
            pltpu.VMEM(shape, f32),
            pltpu.VMEM((12, FULL, 2, 8, 128), f32),
            pltpu.VMEM((12, FULL, 2, 8, 128), f32),
            pltpu.VMEM((12, FULL, 2, 8, 128), f32),
            pltpu.VMEM((4, FULL, 2, 8, 128), f32),
            pltpu.VMEM((6, 9, 2, 8, 128), f32),
            pltpu.VMEM(shape, f32),
        ]
        + [pltpu.VMEM((ROWS2, 2, 8, 128), f32)] * 4
        + [pltpu.VMEM((ROWS2, 8, 128), f32)] * 2
        + [pltpu.VMEM((6, 2, 8, 128), f32)]
        + [pltpu.VMEM((FULL, 2, 8, 128), f32)] * 4
        + [pltpu.VMEM((FULL, 8, 128), f32)] * 2
        + [pltpu.VMEM((6, 2, 8, 128), f32)]
        + [pltpu.VMEM((FULL, 2, 8, 128), f32)] * 2
        + [pltpu.VMEM((FULL, 8, 128), f32)]
        + [
            pltpu.SemaphoreType.DMA((4,)),
            pltpu.SemaphoreType.DMA((4,)),
            pltpu.SemaphoreType.DMA((12,)),
            pltpu.SemaphoreType.DMA((12,)),
        ],
        compiler_params=pltpu.CompilerParams(collective_id=0, has_side_effects=True),
        name="force",
    )(links.reshape(shape))
    return out.reshape(links.shape)


def solution(mesh):
    return jax.shard_map(
        per_device,
        mesh=mesh,
        in_specs=(P(None, None, None, None, "ta", "gz", "gx"),),
        out_specs=P(None, None, None, None, "ta", "gz", "gx"),
        check_vma=False,
    )
```

```python
import jax
import jax.numpy as jnp
from jax import lax
from jax.experimental import pallas as pl
from jax.experimental.pallas import tpu as pltpu
from jax.sharding import PartitionSpec as P

COEFF = -1.9
MESH = pl.DeviceIdType.MESH
AXES = ("ta", "gz", "gx")
ROWS2 = 12
FULL = 18
CORNERS = ((0, 1), (0, 2), (1, 0), (1, 2), (2, 0), (2, 1))


def rs(v, k):
    k = k % 8
    return v if k == 0 else pltpu.roll(v, k, axis=0)


def rl(v, k):
    k = k % 128
    return v if k == 0 else pltpu.roll(v, k, axis=1)


def sublane():
    return lax.broadcasted_iota(jnp.int32, (8, 128), 0)


def lanes():
    return lax.broadcasted_iota(jnp.int32, (8, 128), 1)


def total(terms):
    out = terms[0]
    for t in terms[1:]:
        out = out + t
    return out


def mul_nn(a, b):
    return [
        [
            (
                total([a[i][k][0] * b[k][j][0] for k in range(3)])
                - total([a[i][k][1] * b[k][j][1] for k in range(3)]),
                total([a[i][k][0] * b[k][j][1] for k in range(3)])
                + total([a[i][k][1] * b[k][j][0] for k in range(3)]),
            )
            for j in range(3)
        ]
        for i in range(3)
    ]


def mul_hn(a, b):
    return [
        [
            (
                total([a[k][i][0] * b[k][j][0] for k in range(3)])
                + total([a[k][i][1] * b[k][j][1] for k in range(3)]),
                total([a[k][i][0] * b[k][j][1] for k in range(3)])
                - total([a[k][i][1] * b[k][j][0] for k in range(3)]),
            )
            for j in range(3)
        ]
        for i in range(3)
    ]


def mul_nh(a, b):
    return [
        [
            (
                total([a[i][k][0] * b[j][k][0] for k in range(3)])
                + total([a[i][k][1] * b[j][k][1] for k in range(3)]),
                total([a[i][k][1] * b[j][k][0] for k in range(3)])
                - total([a[i][k][0] * b[j][k][1] for k in range(3)]),
            )
            for j in range(3)
        ]
        for i in range(3)
    ]


def third_row(m):
    row = []
    for col in range(3):
        n, q = (col + 1) % 3, (col + 2) % 3
        r0n, i0n = m[0][n]
        r0q, i0q = m[0][q]
        r1n, i1n = m[1][n]
        r1q, i1q = m[1][q]
        row.append(
            (
                (r0n * r1q - i0n * i1q) - (r0q * r1n - i0q * i1n),
                (r0q * i1n + i0q * r1n) - (r0n * i1q + i0n * r1q),
            )
        )
    return row


def anti(w):
    nine = [w[i][i][1] + w[i][i][1] for i in range(3)]
    for i in range(3):
        for j in range(i + 1, 3):
            nine += [w[i][j][0] - w[j][i][0], w[i][j][1] + w[j][i][1]]
    return nine


def gather(entry, rows=3):
    return [[(entry(i * 6 + j), entry(i * 6 + 3 + j)) for j in range(3)] for i in range(rows)]


def scatter(put, m, first=0):
    for i, row in enumerate(m):
        for j, (re, im) in enumerate(row):
            put((first + i) * 6 + j, re)
            put((first + i) * 6 + 3 + j, im)


def kernel(
    x_hbm, o, u, v, p, l, a,
    sf, sb, sc, hf, hb, hc, far, near, lh,
    in_sem, send_sem, recv_sem,
):
    me = {axis: lax.axis_index(axis) for axis in AXES}
    size = {axis: lax.axis_size(axis) for axis in AXES}
    beside = {
        (d, step): lax.rem(me[AXES[d]] + (step + size[AXES[d]]), size[AXES[d]])
        for d in range(3)
        for step in (-1, 1)
    }

    def at(*steps):
        return {AXES[d]: beside[d, step] for d, step in steps}

    barrier = pltpu.get_barrier_semaphore()
    targets = [at((d, step)) for d in range(3) for step in (-1, 1)]
    targets += [at((back, 1), (ahead, -1)) for back, ahead in CORNERS]
    for target in targets:
        pl.semaphore_signal(barrier, inc=1, device_id=target, device_id_type=MESH)

    loads = [pltpu.make_async_copy(x_hbm.at[d], u.at[d], in_sem.at[d]) for d in range(4)]
    for load in loads:
        load.start()
    for load in loads:
        load.wait()

    def link(d, c, h):
        return u[d, (c // 3) % 2, c // 6, c % 3, h]

    sub, lane = sublane(), lanes()
    low = sub < 4
    zrow = lax.rem(sub, 4)
    group = lax.div(lane, 16)
    slot = lax.rem(group, 4)
    xcol = lax.rem(lane, 16)

    for c in range(ROWS2):
        for pair in range(2):
            sf[pair, c] = jnp.where(low, link(2 * pair, c, 0), rs(link(2 * pair + 1, c, 0), 4))
            sb[pair, c] = jnp.where(low, rs(link(2 * pair, c, 1), 4), link(2 * pair + 1, c, 1))
        for h in range(2):
            first, last = link(0, c, h), rs(link(0, c, h), -3)
            for k in range(1, 4):
                first = jnp.where(zrow == k, rs(link(k, c, h), k), first)
                last = jnp.where(zrow == k, rs(link(k, c, h), k - 3), last)
            sf[2 + h, c] = first
            sb[2 + h, c] = last
        first, last = link(0, c, 0), rl(link(0, c, 0), -112)
        for g in range(1, 8):
            first = jnp.where(group == g, rl(link(g % 4, c, g // 4), 16 * g), first)
            last = jnp.where(group == g, rl(link(g % 4, c, g // 4), 16 * (g - 7)), last)
        sf[4, c] = first
        sb[4, c] = last

    def merged(items):
        out = items[0][1]
        for mask, value in items[1:]:
            out = jnp.where(mask, value, out)
        return out

    for w in range(2):
        six = range(6)
        sc[0, w] = merged([(sub == r, rs(link(0, w * 6 + r, 1), r - 4)) for r in six])
        sc[1, w] = merged([(group == g, rl(link(0, w * 6 + g, 1), 16 * g)) for g in six])
        sc[2, w] = merged([(sub == r, rs(link(1, w * 6 + r, 0), r - 3)) for r in six])
        sc[3, w] = merged(
            [
                ((group == g) & (zrow == t), rl(rs(link(1, t * 6 + g, w), t - 3), 16 * g))
                for t in range(2)
                for g in six
            ]
        )
        sc[4, w] = merged([(group == g, rl(link(2, w * 6 + g, 0), 16 * (g - 7))) for g in six])
        sc[5, w] = merged(
            [
                ((group == g) & (zrow == t), rl(rs(link(2, t * 6 + g, w), t), 16 * (g - 7)))
                for t in range(2)
                for g in six
            ]
        )

    def send(n, src, dst, target):
        return pltpu.make_async_remote_copy(
            src_ref=src,
            dst_ref=dst,
            send_sem=send_sem.at[n],
            recv_sem=recv_sem.at[n],
            device_id=target,
            device_id_type=MESH,
        )

    corner = [
        send(6 + n, sc.at[n], hc.at[n], at((back, 1), (ahead, -1)))
        for n, (back, ahead) in enumerate(CORNERS)
    ]
    tiles = (pl.ds(0, 2), pl.ds(2, 2), pl.ds(4, 1))
    two = pl.ds(0, ROWS2)
    ahead_faces = [
        send(d, sf.at[tiles[d]], hf.at[tiles[d], two], at((d, -1))) for d in range(3)
    ]
    back_faces = [
        send(3 + d, sb.at[tiles[d]], hb.at[tiles[d], two], at((d, 1))) for d in range(3)
    ]
    pl.semaphore_wait(barrier, len(targets))
    for copy in corner:
        copy.start()
    for d in (1, 0, 2):
        ahead_faces[d].start()
        back_faces[d].start()

    def ahead_x(field):
        return jnp.where(xcol == 15, rl(field, 15), rl(field, -1))

    def products(n, carry):
        pair, h = lax.div(n, 2), lax.rem(n, 2)
        mu = lax.div(pair, 3)
        nu = lax.rem(mu + 1 + lax.rem(pair, 3), 4)
        prod = mul_nn(gather(lambda c: link(mu, c, h)), gather(lambda c: v[pair, c, h]))

        def put_p(c, value):
            p[pair, c, h] = value

        def put_l(c, value):
            l[pair, c, h] = value

        scatter(put_p, prod)
        scatter(put_l, mul_hn(prod, gather(lambda c: link(nu, c, h))))
        return carry

    def plaquettes(n, carry):
        index, h = lax.div(n, 2), lax.rem(n, 2)
        step, mu = lax.div(index, 4), lax.rem(index, 4)
        nu = lax.rem(mu + 1 + step, 4)
        q = mul_nh(
            gather(lambda c: p[mu * 3 + step, c, h]), gather(lambda c: p[nu * 3 + 2 - step, c, h])
        )
        for n, value in enumerate(anti(q)):
            a[index, n, h] = value
        return carry

    def complete(ref, k):
        m = gather(lambda c: ref[k, c], 2)

        def put(c, value):
            ref[k, c] = value

        scatter(put, [third_row(m)], 2)

    def move_x(mu):
        pair = mu * 3 + 2 - mu
        for c in range(FULL):
            for h in range(2):
                field = l[pair, c, h]
                v[pair, c, h] = jnp.where(xcol == 0, rl(field, -15), rl(field, 1))

    for c in range(FULL):
        for j in range(3):
            v[j, c, 0] = jnp.where(low, rs(link(1 + j, c, 0), 4), rs(link(1 + j, c, 1), 4))
            for h in range(2):
                v[9 + j, c, h] = ahead_x(link(j, c, h))
    lax.fori_loop(18, 24, products, 0)
    lax.fori_loop(0, 3, lambda j, carry: products(2 * j, carry), 0)

    ahead_faces[2].wait_recv()
    complete(hf, 4)
    for c in range(FULL):
        for j in range(3):
            for h in range(2):
                nu = (3 + j) % 4
                v[6 + j, c, h] = jnp.where(
                    group == 7, rl(hf[4, c], 16 * (7 - h * 4 - nu)), rl(link(nu, c, h), -16)
                )
    lax.fori_loop(12, 18, products, 0)

    ahead_faces[0].wait_recv()
    for k in range(2):
        complete(hf, k)
    for c in range(FULL):
        for j in range(3):
            nu = 1 + j
            halo = hf[nu // 2, c]
            v[j, c, 1] = jnp.where(
                low, rs(link(nu, c, 1), 4), halo if nu % 2 else rs(halo, 4)
            )
    lax.fori_loop(0, 3, lambda j, carry: products(2 * j + 1, carry), 0)
    move_x(0)
    move_x(2)
    lax.fori_loop(4, 10, plaquettes, 0)

    ahead_faces[1].wait_recv()
    for k in range(2, 4):
        complete(hf, k)
    for c in range(FULL):
        for j in range(3):
            for h in range(2):
                nu = (2 + j) % 4
                v[3 + j, c, h] = jnp.where(
                    zrow == 3, rs(hf[2 + h, c], 3 - nu), rs(link(nu, c, h), -1)
                )
    lax.fori_loop(6, 12, products, 0)
    move_x(1)
    lax.fori_loop(0, 4, plaquettes, 0)
    lax.fori_loop(10, 12, plaquettes, 0)

    for copy in back_faces + corner:
        copy.wait_recv()
    for k in range(5):
        complete(hb, k)

    def step_t0(c):
        return jnp.where(sub == 7, rs(hc[0, c // 6], 7 - c % 6), rs(hb[0, c], 3))

    def step_t1(c):
        field = hb[0, c]
        edge = rl(rs(hc[1, c // 6], 4), 16 * (7 - c % 6))
        return jnp.where(
            low, jnp.where(group == 7, edge, rl(field, -16)), ahead_x(rs(field, 4))
        )

    def step_z(h):
        def step(c):
            field = hb[2 + h, c]
            if h == 0:
                along_t = jnp.where(low, rs(field, 3), rs(hb[3, c], 3))
            else:
                along_t = jnp.where(low, rs(field, 3), rs(hc[2, c // 6], 4 - c % 6))
            edge = rl(rs(hc[3, h], 2 - c // 6), 16 * (7 - c % 6))
            along_y = jnp.where(group == 7, edge, rl(rs(field, 1), -16))
            along_x = ahead_x(rs(field, 2))
            return jnp.where(zrow == 0, along_t, jnp.where(zrow == 3, along_x, along_y))

        return step

    def step_y(c):
        field = hb[4, c]
        turned = rs(field, 4)
        edge = rs(rl(hc[4, c // 6], 16 * (4 - c % 6)), 4)
        high = jnp.where(group == 4, edge, rl(turned, 32))
        along_t = jnp.where(low, rl(turned, -32), high)
        edge0 = rs(rl(hc[5, 0], 16 * (1 - c % 6)), 3 - c // 6)
        edge1 = rs(rl(hc[5, 1], 16 * (5 - c % 6)), 3 - c // 6)
        along_z = jnp.where(
            zrow == 3, jnp.where(group == 1, edge0, edge1), rl(rs(field, -1), -16)
        )
        along_x = rl(ahead_x(field), 16)
        return jnp.where(slot == 0, along_t, jnp.where(slot == 3, along_x, along_z))

    for k, step in enumerate((step_t0, step_t1, step_z(0), step_z(1), step_y)):
        m = gather(step, 2)

        def put_far(c, value):
            far[k, c] = value

        scatter(put_far, m + [third_row(m)])
    for c in range(FULL):
        field = hb[0, c]
        near[0, c] = jnp.where(low, field, rs(field, 4))
        near[1, c] = jnp.where(low, field, rs(field, 4))
        for h in range(2):
            field = hb[2 + h, c]
            near[2 + h, c] = jnp.where(
                zrow == 0,
                rs(field, -1),
                jnp.where(zrow == 2, rs(field, 1), jnp.where(zrow == 3, rs(field, 2), field)),
            )
        field = hb[4, c]
        near[4, c] = jnp.where(
            slot == 0,
            rl(field, -32),
            jnp.where(slot == 1, rl(field, -16), jnp.where(slot == 3, rl(field, 16), field)),
        )

    def faces(k, carry):
        prod = mul_nn(gather(lambda c: hb[k, c]), gather(lambda c: far[k, c]))

        def put(c, value):
            lh[k, c] = value

        scatter(put, mul_hn(prod, gather(lambda c: near[k, c])))
        return carry

    lax.fori_loop(0, 5, faces, 0)

    for c in range(FULL):
        for mu in range(4):
            if mu != 0:
                pair = mu * 3 + 3 - mu
                halo = lh[mu // 2, c]
                turned = rs(l[pair, c, 0], 4)
                v[pair, c, 0] = jnp.where(low, rs(halo, 4) if mu % 2 else halo, turned)
                v[pair, c, 1] = jnp.where(low, turned, rs(l[pair, c, 1], 4))
            for h in range(2):
                if mu != 1:
                    pair = mu * 3 + (0 - mu) % 4
                    v[pair, c, h] = jnp.where(
                        zrow == 0, rs(lh[2 + h, c], -mu), rs(l[pair, c, h], 1)
                    )
                if mu != 2:
                    pair = mu * 3 + (1 - mu) % 4
                    v[pair, c, h] = jnp.where(
                        group == 0, rl(lh[4, c], -16 * (h * 4 + mu)), rl(l[pair, c, h], 16)
                    )

    def forces(n, carry):
        mu, h = lax.div(n, 2), lax.rem(n, 2)
        staple = gather(
            lambda c: v[mu * 3, c, h] + v[mu * 3 + 1, c, h] + v[mu * 3 + 2, c, h]
        )
        w = anti(mul_nn(gather(lambda c: link(mu, c, h)), staple))
        prev = lax.rem(mu + 3, 4)
        pick = 4 + lax.rem(mu, 2)
        sign = 1.0 - 2.0 * lax.div(mu, 2).astype(jnp.float32)
        nine = [
            w[k] + (a[mu, k, h] - a[prev, k, h] + sign * a[pick, k, h]) for k in range(9)
        ]
        third = (nine[0] + nine[1] + nine[2]) * (1.0 / 3.0)
        k = 3
        for i in range(3):
            o[mu, 0, i, i, h] = jnp.zeros((8, 128), jnp.float32)
            o[mu, 1, i, i, h] = (0.5 * COEFF) * (nine[i] - third)
            for j in range(i + 1, 3):
                re, im = (0.5 * COEFF) * nine[k], (0.5 * COEFF) * nine[k + 1]
                o[mu, 0, i, j, h] = re
                o[mu, 0, j, i, h] = -re
                o[mu, 1, i, j, h] = im
                o[mu, 1, j, i, h] = im
                k += 2
        return carry

    lax.fori_loop(0, 8, forces, 0)
    for copy in ahead_faces + back_faces + corner:
        copy.wait_send()


def per_device(links):
    shape = (4, 2, 3, 3, 2, 8, 128)

    def vmem(*lead):
        return pltpu.VMEM(lead + (8, 128), jnp.float32)

    pairs = vmem(12, FULL, 2)
    out = pl.pallas_call(
        kernel,
        out_shape=jax.ShapeDtypeStruct(shape, jnp.float32),
        in_specs=[pl.BlockSpec(memory_space=pltpu.HBM)],
        out_specs=pl.BlockSpec(memory_space=pltpu.VMEM),
        scratch_shapes=[
            vmem(4, 2, 3, 3, 2),
            pairs,
            pairs,
            pairs,
            vmem(6, 9, 2),
            vmem(5, ROWS2),
            vmem(5, ROWS2),
            vmem(6, 2),
            vmem(5, FULL),
            vmem(5, FULL),
            vmem(6, 2),
            vmem(5, FULL),
            vmem(5, FULL),
            vmem(5, FULL),
            pltpu.SemaphoreType.DMA((4,)),
            pltpu.SemaphoreType.DMA((12,)),
            pltpu.SemaphoreType.DMA((12,)),
        ],
        compiler_params=pltpu.CompilerParams(
            collective_id=0, has_side_effects=True, vmem_limit_bytes=16 * 1024 * 1024
        ),
        name="force",
    )(pltpu.with_memory_space_constraint(links.reshape(shape), pltpu.HBM))
    return out.reshape(links.shape)


def solution(mesh):
    return jax.shard_map(
        per_device,
        mesh=mesh,
        in_specs=(P(None, None, None, None, "ta", "gz", "gx"),),
        out_specs=P(None, None, None, None, "ta", "gz", "gx"),
        check_vma=False,
    )
```

```python
import jax
import jax.numpy as jnp
from jax import lax
from jax.experimental import pallas as pl
from jax.experimental.pallas import tpu as pltpu
from jax.sharding import PartitionSpec as P

COEFF = -1.9
MESH = pl.DeviceIdType.MESH
AXES = ("ta", "gz", "gx")
ROWS2 = 12
FULL = 18
CORNERS = ((0, 1), (0, 2), (1, 0), (1, 2), (2, 0), (2, 1))


def rs(v, k):
    k = k % 8
    return v if k == 0 else pltpu.roll(v, k, axis=0)


def rl(v, k):
    k = k % 128
    return v if k == 0 else pltpu.roll(v, k, axis=1)


def sublane():
    return lax.broadcasted_iota(jnp.int32, (8, 128), 0)


def lanes():
    return lax.broadcasted_iota(jnp.int32, (8, 128), 1)


def total(terms):
    out = terms[0]
    for t in terms[1:]:
        out = out + t
    return out


def mul_nn(a, b):
    return [
        [
            (
                total([a[i][k][0] * b[k][j][0] for k in range(3)])
                - total([a[i][k][1] * b[k][j][1] for k in range(3)]),
                total([a[i][k][0] * b[k][j][1] for k in range(3)])
                + total([a[i][k][1] * b[k][j][0] for k in range(3)]),
            )
            for j in range(3)
        ]
        for i in range(3)
    ]


def mul_hn(a, b):
    return [
        [
            (
                total([a[k][i][0] * b[k][j][0] for k in range(3)])
                + total([a[k][i][1] * b[k][j][1] for k in range(3)]),
                total([a[k][i][0] * b[k][j][1] for k in range(3)])
                - total([a[k][i][1] * b[k][j][0] for k in range(3)]),
            )
            for j in range(3)
        ]
        for i in range(3)
    ]


def mul_nh(a, b):
    return [
        [
            (
                total([a[i][k][0] * b[j][k][0] for k in range(3)])
                + total([a[i][k][1] * b[j][k][1] for k in range(3)]),
                total([a[i][k][1] * b[j][k][0] for k in range(3)])
                - total([a[i][k][0] * b[j][k][1] for k in range(3)]),
            )
            for j in range(3)
        ]
        for i in range(3)
    ]


def third_row(m):
    row = []
    for col in range(3):
        n, q = (col + 1) % 3, (col + 2) % 3
        r0n, i0n = m[0][n]
        r0q, i0q = m[0][q]
        r1n, i1n = m[1][n]
        r1q, i1q = m[1][q]
        row.append(
            (
                (r0n * r1q - i0n * i1q) - (r0q * r1n - i0q * i1n),
                (r0q * i1n + i0q * r1n) - (r0n * i1q + i0n * r1q),
            )
        )
    return row


def anti(w):
    nine = [w[i][i][1] + w[i][i][1] for i in range(3)]
    for i in range(3):
        for j in range(i + 1, 3):
            nine += [w[i][j][0] - w[j][i][0], w[i][j][1] + w[j][i][1]]
    return nine


def gather(entry, rows=3):
    return [[(entry(i * 6 + j), entry(i * 6 + 3 + j)) for j in range(3)] for i in range(rows)]


def scatter(put, m, first=0):
    for i, row in enumerate(m):
        for j, (re, im) in enumerate(row):
            put((first + i) * 6 + j, re)
            put((first + i) * 6 + 3 + j, im)


def kernel(
    x_hbm, o, u, v, p, l, a,
    sf, sb, sc, hf, hb, hc, far, near, lh, staple, below, upper,
    in_sem, send_sem, recv_sem, ready,
):
    me = {axis: lax.axis_index(axis) for axis in AXES}
    size = {axis: lax.axis_size(axis) for axis in AXES}
    beside = {
        (d, step): lax.rem(me[AXES[d]] + (step + size[AXES[d]]), size[AXES[d]])
        for d in range(3)
        for step in (-1, 1)
    }

    def at(*steps):
        return {AXES[d]: beside[d, step] for d, step in steps}

    barrier = pltpu.get_barrier_semaphore()
    targets = [at((d, step)) for d in range(3) for step in (-1, 1)]
    for target in targets:
        pl.semaphore_signal(barrier, inc=1, device_id=target, device_id_type=MESH)

    loads = [pltpu.make_async_copy(x_hbm.at[d], u.at[d], in_sem.at[d]) for d in range(4)]
    for load in loads:
        load.start()
    for load in loads:
        load.wait()

    def link(d, c, h):
        return u[d, (c // 3) % 2, c // 6, c % 3, h]

    sub, lane = sublane(), lanes()
    low = sub < 4
    zrow = lax.rem(sub, 4)
    group = lax.div(lane, 16)
    slot = lax.rem(group, 4)
    xcol = lax.rem(lane, 16)

    for c in range(ROWS2):
        for pair in range(2):
            sf[pair, c] = jnp.where(low, link(2 * pair, c, 0), rs(link(2 * pair + 1, c, 0), 4))
            sb[pair, c] = jnp.where(low, rs(link(2 * pair, c, 1), 4), link(2 * pair + 1, c, 1))
        for h in range(2):
            first, last = link(0, c, h), rs(link(0, c, h), -3)
            for k in range(1, 4):
                first = jnp.where(zrow == k, rs(link(k, c, h), k), first)
                last = jnp.where(zrow == k, rs(link(k, c, h), k - 3), last)
            sf[2 + h, c] = first
            sb[2 + h, c] = last
        first, last = link(0, c, 0), rl(link(0, c, 0), -112)
        for g in range(1, 8):
            first = jnp.where(group == g, rl(link(g % 4, c, g // 4), 16 * g), first)
            last = jnp.where(group == g, rl(link(g % 4, c, g // 4), 16 * (g - 7)), last)
        sf[4, c] = first
        sb[4, c] = last

    def merged(items):
        out = items[0][1]
        for mask, value in items[1:]:
            out = jnp.where(mask, value, out)
        return out

    for w in range(2):
        six = range(6)
        sc[0, w] = merged([(sub == r, rs(link(0, w * 6 + r, 1), r - 4)) for r in six])
        sc[1, w] = merged([(group == g, rl(link(0, w * 6 + g, 1), 16 * g)) for g in six])
        sc[2, w] = merged([(sub == r, rs(link(1, w * 6 + r, 0), r - 3)) for r in six])
        sc[3, w] = merged(
            [
                ((group == g) & (zrow == t), rl(rs(link(1, t * 6 + g, w), t - 3), 16 * g))
                for t in range(2)
                for g in six
            ]
        )
        sc[4, w] = merged([(group == g, rl(link(2, w * 6 + g, 0), 16 * (g - 7))) for g in six])
        sc[5, w] = merged(
            [
                ((group == g) & (zrow == t), rl(rs(link(2, t * 6 + g, w), t), 16 * (g - 7)))
                for t in range(2)
                for g in six
            ]
        )

    def send(n, src, dst, target):
        return pltpu.make_async_remote_copy(
            src_ref=src,
            dst_ref=dst,
            send_sem=send_sem.at[n],
            recv_sem=recv_sem.at[n],
            device_id=target,
            device_id_type=MESH,
        )

    corner = [
        send(6 + n, sc.at[n], hc.at[n], at((back, 1), (ahead, -1)))
        for n, (back, ahead) in enumerate(CORNERS)
    ]
    tiles = (pl.ds(0, 2), pl.ds(2, 2), pl.ds(4, 1))
    two = pl.ds(0, ROWS2)
    ahead_faces = [
        send(d, sf.at[tiles[d]], hf.at[tiles[d], two], at((d, -1))) for d in range(3)
    ]
    back_faces = [
        send(3 + d, sb.at[tiles[d]], hb.at[tiles[d], two], at((d, 1))) for d in range(3)
    ]
    pl.semaphore_wait(barrier, len(targets))
    words = ((0, -1), (0, 1), (2, -1), (2, 1))
    for n, word in enumerate(words):
        pl.semaphore_signal(ready.at[n], inc=1, device_id=at(word), device_id_type=MESH)
    for d in (1, 0, 2):
        back_faces[d].start()
        ahead_faces[d].start()
    for n, through in enumerate(((0,), (2,), (4, 5), (1, 3))):
        pl.semaphore_wait(ready.at[n], 1)
        for m in through:
            corner[m].start()

    def ahead_x(field):
        return jnp.where(xcol == 15, rl(field, 15), rl(field, -1))

    def products(n, carry):
        pair, h = lax.div(n, 2), lax.rem(n, 2)
        mu = lax.div(pair, 3)
        nu = lax.rem(mu + 1 + lax.rem(pair, 3), 4)
        prod = mul_nn(gather(lambda c: link(mu, c, h)), gather(lambda c: v[pair, c, h]))

        def put_p(c, value):
            p[pair, c, h] = value

        def put_l(c, value):
            l[pair, c, h] = value

        scatter(put_p, prod)
        scatter(put_l, mul_hn(prod, gather(lambda c: link(nu, c, h))))
        return carry

    def plaquettes(n, carry):
        index, h = lax.div(n, 2), lax.rem(n, 2)
        step, mu = lax.div(index, 4), lax.rem(index, 4)
        nu = lax.rem(mu + 1 + step, 4)
        q = mul_nh(
            gather(lambda c: p[mu * 3 + step, c, h]), gather(lambda c: p[nu * 3 + 2 - step, c, h])
        )
        for n, value in enumerate(anti(q)):
            a[index, n, h] = value
        return carry

    def complete(ref, k):
        m = gather(lambda c: ref[k, c], 2)

        def put(c, value):
            ref[k, c] = value

        scatter(put, [third_row(m)], 2)

    def move_x(mu):
        pair = mu * 3 + 2 - mu
        for c in range(FULL):
            for h in range(2):
                field = l[pair, c, h]
                v[pair, c, h] = jnp.where(xcol == 0, rl(field, -15), rl(field, 1))

    for c in range(FULL):
        for j in range(3):
            v[j, c, 0] = jnp.where(low, rs(link(1 + j, c, 0), 4), rs(link(1 + j, c, 1), 4))
            for h in range(2):
                v[9 + j, c, h] = ahead_x(link(j, c, h))
    lax.fori_loop(18, 24, products, 0)
    lax.fori_loop(0, 3, lambda j, carry: products(2 * j, carry), 0)

    ahead_faces[2].wait_recv()
    complete(hf, 4)
    for c in range(FULL):
        for j in range(3):
            for h in range(2):
                nu = (3 + j) % 4
                v[6 + j, c, h] = jnp.where(
                    group == 7, rl(hf[4, c], 16 * (7 - h * 4 - nu)), rl(link(nu, c, h), -16)
                )
    lax.fori_loop(12, 18, products, 0)

    ahead_faces[0].wait_recv()
    for k in range(2):
        complete(hf, k)
    for c in range(FULL):
        for j in range(3):
            nu = 1 + j
            halo = hf[nu // 2, c]
            v[j, c, 1] = jnp.where(
                low, rs(link(nu, c, 1), 4), halo if nu % 2 else rs(halo, 4)
            )
    lax.fori_loop(0, 3, lambda j, carry: products(2 * j + 1, carry), 0)
    move_x(0)
    move_x(2)
    lax.fori_loop(4, 10, plaquettes, 0)

    ahead_faces[1].wait_recv()
    for k in range(2, 4):
        complete(hf, k)
    for c in range(FULL):
        for j in range(3):
            for h in range(2):
                nu = (2 + j) % 4
                v[3 + j, c, h] = jnp.where(
                    zrow == 3, rs(hf[2 + h, c], 3 - nu), rs(link(nu, c, h), -1)
                )
    lax.fori_loop(6, 12, products, 0)
    move_x(1)
    lax.fori_loop(0, 4, plaquettes, 0)
    lax.fori_loop(10, 12, plaquettes, 0)

    def step_t0(c):
        return jnp.where(sub == 7, rs(hc[0, c // 6], 7 - c % 6), rs(hb[0, c], 3))

    def step_t1(c):
        field = hb[0, c]
        edge = rl(rs(hc[1, c // 6], 4), 16 * (7 - c % 6))
        return jnp.where(
            low, jnp.where(group == 7, edge, rl(field, -16)), ahead_x(rs(field, 4))
        )

    def step_z(h):
        def step(c):
            field = hb[2 + h, c]
            if h == 0:
                along_t = jnp.where(low, rs(field, 3), rs(hb[3, c], 3))
            else:
                along_t = jnp.where(low, rs(field, 3), rs(hc[2, c // 6], 4 - c % 6))
            edge = rl(rs(hc[3, h], 2 - c // 6), 16 * (7 - c % 6))
            along_y = jnp.where(group == 7, edge, rl(rs(field, 1), -16))
            along_x = ahead_x(rs(field, 2))
            return jnp.where(zrow == 0, along_t, jnp.where(zrow == 3, along_x, along_y))

        return step

    def step_y(c):
        field = hb[4, c]
        turned = rs(field, 4)
        edge = rs(rl(hc[4, c // 6], 16 * (4 - c % 6)), 4)
        high = jnp.where(group == 4, edge, rl(turned, 32))
        along_t = jnp.where(low, rl(turned, -32), high)
        edge0 = rs(rl(hc[5, 0], 16 * (1 - c % 6)), 3 - c // 6)
        edge1 = rs(rl(hc[5, 1], 16 * (5 - c % 6)), 3 - c // 6)
        along_z = jnp.where(
            zrow == 3, jnp.where(group == 1, edge0, edge1), rl(rs(field, -1), -16)
        )
        along_x = rl(ahead_x(field), 16)
        return jnp.where(slot == 0, along_t, jnp.where(slot == 3, along_x, along_z))

    def faces(k, carry):
        prod = mul_nn(gather(lambda c: hb[k, c]), gather(lambda c: far[k, c]))

        def put(c, value):
            lh[k, c] = value

        scatter(put, mul_hn(prod, gather(lambda c: near[k, c])))
        return carry

    def put_far(k, step):
        m = gather(step, 2)

        def put(c, value):
            far[k, c] = value

        scatter(put, m + [third_row(m)])

    def uppers(n, carry):
        mu, h = lax.div(n, 2), lax.rem(n, 2)
        prev = lax.rem(mu + 3, 4)
        pick = 4 + lax.rem(mu, 2)
        sign = 1.0 - 2.0 * lax.div(mu, 2).astype(jnp.float32)
        for k in range(9):
            upper[mu, k, h] = a[mu, k, h] - a[prev, k, h] + sign * a[pick, k, h]
        return carry

    def forces(mu, h, entry):
        w = anti(mul_nn(gather(lambda c: link(mu, c, h)), gather(entry)))
        nine = [w[k] + upper[mu, k, h] for k in range(9)]
        third = (nine[0] + nine[1] + nine[2]) * (1.0 / 3.0)
        k = 3
        for i in range(3):
            o[mu, 0, i, i, h] = jnp.zeros((8, 128), jnp.float32)
            o[mu, 1, i, i, h] = (0.5 * COEFF) * (nine[i] - third)
            for j in range(i + 1, 3):
                re, im = (0.5 * COEFF) * nine[k], (0.5 * COEFF) * nine[k + 1]
                o[mu, 0, i, j, h] = re
                o[mu, 0, j, i, h] = -re
                o[mu, 1, i, j, h] = im
                o[mu, 1, j, i, h] = im
                k += 2

    lax.fori_loop(0, 8, uppers, 0)
    for copy in (back_faces[0], back_faces[2], corner[0], corner[1], corner[4], corner[5]):
        copy.wait_recv()
    for k in (0, 1, 4):
        complete(hb, k)
    put_far(0, step_t0)
    put_far(1, step_t1)
    put_far(4, step_y)
    for c in range(FULL):
        field = hb[0, c]
        both = jnp.where(low, field, rs(field, 4))
        near[0, c] = both
        near[1, c] = both
        field = hb[4, c]
        near[4, c] = jnp.where(
            slot == 0,
            rl(field, -32),
            jnp.where(slot == 1, rl(field, -16), jnp.where(slot == 3, rl(field, 16), field)),
        )
    lax.fori_loop(0, 3, lambda k, carry: faces(k + lax.div(k, 2) * 2, carry), 0)
    for c in range(FULL):
        for mu in range(4):
            for h in range(2):
                terms = []
                if mu != 3:
                    terms.append(v[mu * 3 + 2 - mu, c, h])
                if mu != 0:
                    pair = mu * 3 + 3 - mu
                    turned = rs(l[pair, c, 0], 4)
                    if h == 0:
                        halo = lh[mu // 2, c]
                        moved = jnp.where(low, rs(halo, 4) if mu % 2 else halo, turned)
                    else:
                        moved = jnp.where(low, turned, rs(l[pair, c, 1], 4))
                    terms.append(moved)
                if mu != 2:
                    pair = mu * 3 + (1 - mu) % 4
                    moved = jnp.where(
                        group == 0, rl(lh[4, c], -16 * (h * 4 + mu)), rl(l[pair, c, h], 16)
                    )
                    terms.append(moved)
                staple[mu, c, h] = total(terms)

    def forces_z(h, carry):
        forces(1, h, lambda c: staple[1, c, h])
        return carry

    lax.fori_loop(0, 2, forces_z, 0)

    for copy in (back_faces[1], corner[2], corner[3]):
        copy.wait_recv()
    for k in (2, 3):
        complete(hb, k)
    put_far(2, step_z(0))
    put_far(3, step_z(1))
    for c in range(FULL):
        for h in range(2):
            field = hb[2 + h, c]
            near[2 + h, c] = jnp.where(
                zrow == 0,
                rs(field, -1),
                jnp.where(zrow == 2, rs(field, 1), jnp.where(zrow == 3, rs(field, 2), field)),
            )
    lax.fori_loop(2, 4, faces, 0)
    for c in range(FULL):
        for h in range(2):
            for mu in (0, 2, 3):
                pair = mu * 3 + (0 - mu) % 4
                below[mu, c, h] = jnp.where(
                    zrow == 0, rs(lh[2 + h, c], -mu), rs(l[pair, c, h], 1)
                )

    def forces_rest(n, carry):
        m, h = lax.div(n, 2), lax.rem(n, 2)
        mu = m + lax.div(m + 1, 2)
        forces(mu, h, lambda c: staple[mu, c, h] + below[mu, c, h])
        return carry

    lax.fori_loop(0, 6, forces_rest, 0)
    for copy in ahead_faces + back_faces + corner:
        copy.wait_send()


def per_device(links):
    shape = (4, 2, 3, 3, 2, 8, 128)

    def vmem(*lead):
        return pltpu.VMEM(lead + (8, 128), jnp.float32)

    pairs = vmem(12, FULL, 2)
    out = pl.pallas_call(
        kernel,
        out_shape=jax.ShapeDtypeStruct(shape, jnp.float32),
        in_specs=[pl.BlockSpec(memory_space=pltpu.HBM)],
        out_specs=pl.BlockSpec(memory_space=pltpu.VMEM),
        scratch_shapes=[
            vmem(4, 2, 3, 3, 2),
            pairs,
            pairs,
            pairs,
            vmem(6, 9, 2),
            vmem(5, ROWS2),
            vmem(5, ROWS2),
            vmem(6, 2),
            vmem(5, FULL),
            vmem(5, FULL),
            vmem(6, 2),
            vmem(5, FULL),
            vmem(5, FULL),
            vmem(5, FULL),
            vmem(4, FULL, 2),
            vmem(4, FULL, 2),
            vmem(4, 9, 2),
            pltpu.SemaphoreType.DMA((4,)),
            pltpu.SemaphoreType.DMA((12,)),
            pltpu.SemaphoreType.DMA((12,)),
            pltpu.SemaphoreType.REGULAR((4,)),
        ],
        compiler_params=pltpu.CompilerParams(
            collective_id=0, has_side_effects=True, vmem_limit_bytes=16 * 1024 * 1024
        ),
        name="force",
    )(pltpu.with_memory_space_constraint(links.reshape(shape), pltpu.HBM))
    return out.reshape(links.shape)


def solution(mesh):
    return jax.shard_map(
        per_device,
        mesh=mesh,
        in_specs=(P(None, None, None, None, "ta", "gz", "gx"),),
        out_specs=P(None, None, None, None, "ta", "gz", "gx"),
        check_vma=False,
    )
```

```python
import jax
import jax.numpy as jnp
from jax import lax
from jax.experimental import pallas as pl
from jax.experimental.pallas import tpu as pltpu
from jax.sharding import PartitionSpec as P

COEFF = -1.9
MESH = pl.DeviceIdType.MESH
AXES = ("ta", "gz", "gx")
ROWS2 = 12
FULL = 18
CORNERS = ((0, 1), (0, 2), (1, 0), (1, 2), (2, 0), (2, 1))


def rs(v, k):
    k = k % 8
    return v if k == 0 else pltpu.roll(v, k, axis=0)


def rl(v, k):
    k = k % 128
    return v if k == 0 else pltpu.roll(v, k, axis=1)


def sublane():
    return lax.broadcasted_iota(jnp.int32, (8, 128), 0)


def lanes():
    return lax.broadcasted_iota(jnp.int32, (8, 128), 1)


def pick(v, index):
    return jnp.take_along_axis(v, index, axis=1, mode="promise_in_bounds")


def total(terms):
    out = terms[0]
    for t in terms[1:]:
        out = out + t
    return out


def mul_nn(a, b):
    return [
        [
            (
                total([a[i][k][0] * b[k][j][0] for k in range(3)])
                - total([a[i][k][1] * b[k][j][1] for k in range(3)]),
                total([a[i][k][0] * b[k][j][1] for k in range(3)])
                + total([a[i][k][1] * b[k][j][0] for k in range(3)]),
            )
            for j in range(3)
        ]
        for i in range(3)
    ]


def mul_hn(a, b):
    return [
        [
            (
                total([a[k][i][0] * b[k][j][0] for k in range(3)])
                + total([a[k][i][1] * b[k][j][1] for k in range(3)]),
                total([a[k][i][0] * b[k][j][1] for k in range(3)])
                - total([a[k][i][1] * b[k][j][0] for k in range(3)]),
            )
            for j in range(3)
        ]
        for i in range(3)
    ]


def mul_nh(a, b):
    return [
        [
            (
                total([a[i][k][0] * b[j][k][0] for k in range(3)])
                + total([a[i][k][1] * b[j][k][1] for k in range(3)]),
                total([a[i][k][1] * b[j][k][0] for k in range(3)])
                - total([a[i][k][0] * b[j][k][1] for k in range(3)]),
            )
            for j in range(3)
        ]
        for i in range(3)
    ]


def third_row(m):
    row = []
    for col in range(3):
        n, q = (col + 1) % 3, (col + 2) % 3
        r0n, i0n = m[0][n]
        r0q, i0q = m[0][q]
        r1n, i1n = m[1][n]
        r1q, i1q = m[1][q]
        row.append(
            (
                (r0n * r1q - i0n * i1q) - (r0q * r1n - i0q * i1n),
                (r0q * i1n + i0q * r1n) - (r0n * i1q + i0n * r1q),
            )
        )
    return row


def anti(w):
    nine = [w[i][i][1] + w[i][i][1] for i in range(3)]
    for i in range(3):
        for j in range(i + 1, 3):
            nine += [w[i][j][0] - w[j][i][0], w[i][j][1] + w[j][i][1]]
    return nine


def gather(entry, rows=3):
    return [[(entry(i * 6 + j), entry(i * 6 + 3 + j)) for j in range(3)] for i in range(rows)]


def scatter(put, m, first=0):
    for i, row in enumerate(m):
        for j, (re, im) in enumerate(row):
            put((first + i) * 6 + j, re)
            put((first + i) * 6 + 3 + j, im)


def kernel(
    x_hbm, o, u, v, p, l, a,
    sf, sb, sc, hf, hb, hc, far, near, lh, own, pf, lf, staple, below,
    in_sem, send_sem, recv_sem, ready,
):
    me = {axis: lax.axis_index(axis) for axis in AXES}
    size = {axis: lax.axis_size(axis) for axis in AXES}
    beside = {
        (d, step): lax.rem(me[AXES[d]] + (step + size[AXES[d]]), size[AXES[d]])
        for d in range(3)
        for step in (-1, 1)
    }

    def at(*steps):
        return {AXES[d]: beside[d, step] for d, step in steps}

    barrier = pltpu.get_barrier_semaphore()
    targets = [at((d, step)) for d in range(3) for step in (-1, 1)]
    for target in targets:
        pl.semaphore_signal(barrier, inc=1, device_id=target, device_id_type=MESH)

    loads = [pltpu.make_async_copy(x_hbm.at[d], u.at[d], in_sem.at[d]) for d in range(4)]
    for load in loads:
        load.start()
    for load in loads:
        load.wait()

    def link(d, c, h):
        return u[d, (c // 3) % 2, c // 6, c % 3, h]

    sub, lane = sublane(), lanes()
    low = sub < 4
    zrow = lax.rem(sub, 4)
    group = lax.div(lane, 16)
    slot = lax.rem(group, 4)
    xcol = lax.rem(lane, 16)
    row16 = lane - xcol
    to_next = row16 + lax.rem(xcol + 1, 16)
    to_last = row16 + lax.rem(xcol + 15, 16)
    own_row = lax.div(lane, 64) * 64 + 32 + xcol
    next_x = lax.rem(row16 + 112, 128) + lax.rem(xcol + 1, 16)
    time_row = lax.rem(lane + jnp.where(low, 32, 96), 128)

    for c in range(FULL):
        for pair in range(2):
            even, odd = 2 * pair, 2 * pair + 1
            sb[pair, c] = jnp.where(low, rs(link(even, c, 1), 4), link(odd, c, 1))
            if c < ROWS2:
                sf[pair, c] = jnp.where(low, link(even, c, 0), rs(link(odd, c, 0), 4))
        for h in range(2):
            last = rs(link(0, c, h), -3)
            for k in range(1, 4):
                last = jnp.where(zrow == k, rs(link(k, c, h), k - 3), last)
            sb[2 + h, c] = last
            if c < ROWS2:
                first = link(0, c, h)
                for k in range(1, 4):
                    first = jnp.where(zrow == k, rs(link(k, c, h), k), first)
                sf[2 + h, c] = first
        last = rl(link(0, c, 0), -112)
        for g in range(1, 8):
            last = jnp.where(group == g, rl(link(g % 4, c, g // 4), 16 * (g - 7)), last)
        sb[4, c] = last
        if c < ROWS2:
            first = link(0, c, 0)
            for g in range(1, 8):
                first = jnp.where(group == g, rl(link(g % 4, c, g // 4), 16 * g), first)
            sf[4, c] = first

    def merged(items):
        out = items[0][1]
        for mask, value in items[1:]:
            out = jnp.where(mask, value, out)
        return out

    for w in range(2):
        six = range(6)
        sc[0, w] = merged([(sub == r, rs(link(0, w * 6 + r, 1), r - 4)) for r in six])
        sc[1, w] = merged([(group == g, rl(link(0, w * 6 + g, 1), 16 * g)) for g in six])
        sc[2, w] = merged([(sub == r, rs(link(1, w * 6 + r, 0), r - 3)) for r in six])
        sc[3, w] = merged(
            [
                ((group == g) & (zrow == t), rl(rs(link(1, t * 6 + g, w), t - 3), 16 * g))
                for t in range(2)
                for g in six
            ]
        )
        sc[4, w] = merged([(group == g, rl(link(2, w * 6 + g, 0), 16 * (g - 7))) for g in six])
        sc[5, w] = merged(
            [
                ((group == g) & (zrow == t), rl(rs(link(2, t * 6 + g, w), t), 16 * (g - 7)))
                for t in range(2)
                for g in six
            ]
        )

    def send(n, src, dst, target):
        return pltpu.make_async_remote_copy(
            src_ref=src,
            dst_ref=dst,
            send_sem=send_sem.at[n],
            recv_sem=recv_sem.at[n],
            device_id=target,
            device_id_type=MESH,
        )

    corner = [
        send(6 + n, sc.at[n], hc.at[n], at((back, 1), (ahead, -1)))
        for n, (back, ahead) in enumerate(CORNERS)
    ]
    tiles = (pl.ds(0, 2), pl.ds(2, 2), pl.ds(4, 1))
    two = pl.ds(0, ROWS2)
    ahead_faces = [
        send(d, sf.at[tiles[d]], hf.at[tiles[d], two], at((d, -1))) for d in range(3)
    ]
    back_faces = [
        send(3 + d, sb.at[tiles[d], two], hb.at[tiles[d], two], at((d, 1))) for d in range(3)
    ]
    pl.semaphore_wait(barrier, len(targets))
    words = ((0, -1), (0, 1), (2, -1), (2, 1))
    for n, word in enumerate(words):
        pl.semaphore_signal(ready.at[n], inc=1, device_id=at(word), device_id_type=MESH)
    for d in (1, 0, 2):
        back_faces[d].start()
        ahead_faces[d].start()
    for n, through in enumerate(((0,), (2,), (4, 5), (1, 3))):
        pl.semaphore_wait(ready.at[n], 1)
        for m in through:
            corner[m].start()

    def ahead_x(field):
        return pick(field, to_next)

    def products(n, carry):
        pair, h = lax.div(n, 2), lax.rem(n, 2)
        mu = lax.div(pair, 3)
        nu = lax.rem(mu + 1 + lax.rem(pair, 3), 4)
        prod = mul_nn(gather(lambda c: link(mu, c, h)), gather(lambda c: v[pair, c, h]))

        def put_p(c, value):
            p[pair, c, h] = value

        def put_l(c, value):
            l[pair, c, h] = value

        scatter(put_p, prod)
        scatter(put_l, mul_hn(prod, gather(lambda c: link(nu, c, h))))
        return carry

    def plaquettes(n, carry):
        index, h = lax.div(n, 2), lax.rem(n, 2)
        step, mu = lax.div(index, 4), lax.rem(index, 4)
        nu = lax.rem(mu + 1 + step, 4)
        q = mul_nh(
            gather(lambda c: p[mu * 3 + step, c, h]), gather(lambda c: p[nu * 3 + 2 - step, c, h])
        )
        for n, value in enumerate(anti(q)):
            a[index, n, h] = value
        return carry

    def complete(ref, k):
        m = gather(lambda c: ref[k, c], 2)

        def put(c, value):
            ref[k, c] = value

        scatter(put, [third_row(m)], 2)

    def last_products(k, carry):
        prod = mul_nn(gather(lambda c: own[k, c]), gather(lambda c: hf[k, c]))

        def put_p(c, value):
            pf[k, c] = value

        def put_l(c, value):
            lf[k, c] = value

        scatter(put_p, prod)
        scatter(put_l, mul_hn(prod, gather(lambda c: sb[k, c])))
        return carry

    def spread_z(field):
        return jnp.where(
            zrow == 0,
            rs(field, -1),
            jnp.where(zrow == 2, rs(field, 1), jnp.where(zrow == 3, rs(field, 2), field)),
        )

    for c in range(FULL):
        for j in range(3):
            v[j, c, 0] = jnp.where(low, rs(link(1 + j, c, 0), 4), rs(link(1 + j, c, 1), 4))
            for h in range(2):
                v[3 + j, c, h] = rs(link((2 + j) % 4, c, h), -1)
                v[6 + j, c, h] = rl(link((3 + j) % 4, c, h), -16)
                v[9 + j, c, h] = ahead_x(link(j, c, h))
        for h in range(2):
            own[2 + h, c] = spread_z(sb[2 + h, c])
        own[4, c] = pick(sb[4, c], own_row)
    lax.fori_loop(6, 24, products, 0)
    lax.fori_loop(0, 3, lambda j, carry: products(2 * j, carry), 0)
    for c in range(FULL):
        v[2, c, 0] = pick(l[2, c, 0], to_last)
        v[1, c, 0] = rl(l[1, c, 0], 16)
        for h in range(2):
            v[4, c, h] = pick(l[4, c, h], to_last)
            v[6, c, h] = pick(l[6, c, h], to_last)
            v[11, c, h] = rl(l[11, c, h], 16)

    ahead_faces[2].wait_recv()
    complete(hf, 4)
    lax.fori_loop(4, 5, last_products, 0)
    for c in range(FULL):
        for j in range(3):
            nu = (3 + j) % 4
            for h in range(2):
                turn = 16 * (7 - h * 4 - nu)
                p[6 + j, c, h] = jnp.where(group == 7, rl(pf[4, c], turn), p[6 + j, c, h])
                if j == 0:
                    moved = pick(lf[4, c], 16 * (h * 4 + nu) + lax.rem(xcol + 15, 16))
                    v[6, c, h] = jnp.where(group == 7, moved, v[6, c, h])
                else:
                    l[6 + j, c, h] = jnp.where(group == 7, rl(lf[4, c], turn), l[6 + j, c, h])

    ahead_faces[0].wait_recv()
    for k in range(2):
        complete(hf, k)
    for c in range(FULL):
        for j in range(3):
            nu = 1 + j
            halo = hf[nu // 2, c]
            v[j, c, 1] = jnp.where(
                low, rs(link(nu, c, 1), 4), halo if nu % 2 else rs(halo, 4)
            )
    lax.fori_loop(0, 3, lambda j, carry: products(2 * j + 1, carry), 0)
    for c in range(FULL):
        v[2, c, 1] = pick(l[2, c, 1], to_last)
        v[1, c, 1] = rl(l[1, c, 1], 16)
    lax.fori_loop(4, 10, plaquettes, 0)

    ahead_faces[1].wait_recv()
    for k in range(2, 4):
        complete(hf, k)
    lax.fori_loop(2, 4, last_products, 0)
    for c in range(FULL):
        for j in range(3):
            nu = (2 + j) % 4
            for h in range(2):
                p[3 + j, c, h] = jnp.where(zrow == 3, rs(pf[2 + h, c], 3 - nu), p[3 + j, c, h])
                if j == 1:
                    v[4, c, h] = jnp.where(zrow == 3, pick(lf[2 + h, c], to_last), v[4, c, h])
                else:
                    l[3 + j, c, h] = jnp.where(
                        zrow == 3, rs(lf[2 + h, c], 3 - nu), l[3 + j, c, h]
                    )
    lax.fori_loop(0, 4, plaquettes, 0)
    lax.fori_loop(10, 12, plaquettes, 0)

    def step_t0(c):
        return jnp.where(sub == 7, rs(hc[0, c // 6], 7 - c % 6), rs(hb[0, c], 3))

    def step_t1(c):
        field = hb[0, c]
        edge = rl(rs(hc[1, c // 6], 4), 16 * (7 - c % 6))
        return jnp.where(
            low, jnp.where(group == 7, edge, rl(field, -16)), ahead_x(rs(field, 4))
        )

    def step_z(h):
        def step(c):
            field = hb[2 + h, c]
            if h == 0:
                along_t = jnp.where(low, rs(field, 3), rs(hb[3, c], 3))
            else:
                along_t = jnp.where(low, rs(field, 3), rs(hc[2, c // 6], 4 - c % 6))
            edge = rl(rs(hc[3, h], 2 - c // 6), 16 * (7 - c % 6))
            along_y = jnp.where(group == 7, edge, rl(rs(field, 1), -16))
            along_x = ahead_x(rs(field, 2))
            return jnp.where(zrow == 0, along_t, jnp.where(zrow == 3, along_x, along_y))

        return step

    def step_y(c):
        field = hb[4, c]
        turned = rs(field, 4)
        edge = rs(rl(hc[4, c // 6], 16 * (4 - c % 6)), 4)
        along_t = jnp.where((group == 4) & (sub >= 4), edge, pick(turned, time_row))
        edge0 = rs(rl(hc[5, 0], 16 * (1 - c % 6)), 3 - c // 6)
        edge1 = rs(rl(hc[5, 1], 16 * (5 - c % 6)), 3 - c // 6)
        along_z = jnp.where(
            zrow == 3, jnp.where(group == 1, edge0, edge1), rl(rs(field, -1), -16)
        )
        along_x = pick(field, next_x)
        return jnp.where(slot == 0, along_t, jnp.where(slot == 3, along_x, along_z))

    def faces(k, carry):
        prod = mul_nn(gather(lambda c: hb[k, c]), gather(lambda c: far[k, c]))

        def put(c, value):
            lh[k, c] = value

        scatter(put, mul_hn(prod, gather(lambda c: near[k, c])))
        return carry

    def put_far(k, step):
        m = gather(step, 2)

        def put(c, value):
            far[k, c] = value

        scatter(put, m + [third_row(m)])

    def forces(mu, h, entry):
        w = anti(mul_nn(gather(lambda c: link(mu, c, h)), gather(entry)))
        prev, other = lax.rem(mu + 3, 4), 4 + lax.rem(mu, 2)
        sign = 1.0 - 2.0 * lax.div(mu, 2).astype(jnp.float32)
        nine = [
            w[k] + (a[mu, k, h] - a[prev, k, h] + sign * a[other, k, h]) for k in range(9)
        ]
        third = (nine[0] + nine[1] + nine[2]) * (1.0 / 3.0)
        k = 3
        for i in range(3):
            o[mu, 0, i, i, h] = jnp.zeros((8, 128), jnp.float32)
            o[mu, 1, i, i, h] = (0.5 * COEFF) * (nine[i] - third)
            for j in range(i + 1, 3):
                re, im = (0.5 * COEFF) * nine[k], (0.5 * COEFF) * nine[k + 1]
                o[mu, 0, i, j, h] = re
                o[mu, 0, j, i, h] = -re
                o[mu, 1, i, j, h] = im
                o[mu, 1, j, i, h] = im
                k += 2

    for copy in (back_faces[0], back_faces[2], corner[0], corner[1], corner[4], corner[5]):
        copy.wait_recv()
    for k in (0, 1, 4):
        complete(hb, k)
    put_far(0, step_t0)
    put_far(1, step_t1)
    put_far(4, step_y)
    for c in range(FULL):
        field = hb[0, c]
        both = jnp.where(low, field, rs(field, 4))
        near[0, c] = both
        near[1, c] = both
        field = hb[4, c]
        near[4, c] = pick(field, own_row)
    lax.fori_loop(0, 3, lambda k, carry: faces(k + lax.div(k, 2) * 2, carry), 0)
    for c in range(FULL):
        for mu in range(4):
            for h in range(2):
                terms = []
                if mu != 3:
                    terms.append(v[mu * 3 + 2 - mu, c, h])
                if mu != 0:
                    pair = mu * 3 + 3 - mu
                    turned = rs(l[pair, c, 0], 4)
                    if h == 0:
                        halo = lh[mu // 2, c]
                        moved = jnp.where(low, rs(halo, 4) if mu % 2 else halo, turned)
                    else:
                        moved = jnp.where(low, turned, rs(l[pair, c, 1], 4))
                    terms.append(moved)
                if mu != 2:
                    pair = mu * 3 + (1 - mu) % 4
                    moved = rl(l[pair, c, h], 16) if mu == 1 else v[pair, c, h]
                    halo = rl(lh[4, c], -16 * (h * 4 + mu))
                    terms.append(jnp.where(group == 0, halo, moved))
                staple[mu, c, h] = total(terms)

    def forces_z(h, carry):
        forces(jnp.int32(1), h, lambda c: staple[1, c, h])
        return carry

    lax.fori_loop(0, 2, forces_z, 0)

    for copy in (back_faces[1], corner[2], corner[3]):
        copy.wait_recv()
    for k in (2, 3):
        complete(hb, k)
    put_far(2, step_z(0))
    put_far(3, step_z(1))
    for c in range(FULL):
        for h in range(2):
            near[2 + h, c] = spread_z(hb[2 + h, c])
    lax.fori_loop(2, 4, faces, 0)
    for c in range(FULL):
        for h in range(2):
            for mu in (0, 2, 3):
                pair = mu * 3 + (0 - mu) % 4
                below[mu, c, h] = jnp.where(
                    zrow == 0, rs(lh[2 + h, c], -mu), rs(l[pair, c, h], 1)
                )

    def forces_rest(n, carry):
        m, h = lax.div(n, 2), lax.rem(n, 2)
        mu = m + lax.div(m + 1, 2)
        forces(mu, h, lambda c: staple[mu, c, h] + below[mu, c, h])
        return carry

    lax.fori_loop(0, 6, forces_rest, 0)
    for copy in ahead_faces + back_faces + corner:
        copy.wait_send()


def per_device(links):
    shape = (4, 2, 3, 3, 2, 8, 128)

    def vmem(*lead):
        return pltpu.VMEM(lead + (8, 128), jnp.float32)

    pairs = vmem(12, FULL, 2)
    out = pl.pallas_call(
        kernel,
        out_shape=jax.ShapeDtypeStruct(shape, jnp.float32),
        in_specs=[pl.BlockSpec(memory_space=pltpu.HBM)],
        out_specs=pl.BlockSpec(memory_space=pltpu.VMEM),
        scratch_shapes=[
            vmem(4, 2, 3, 3, 2),
            pairs,
            pairs,
            pairs,
            vmem(6, 9, 2),
            vmem(5, ROWS2),
            vmem(5, FULL),
            vmem(6, 2),
            vmem(5, FULL),
            vmem(5, FULL),
            vmem(6, 2),
            vmem(5, FULL),
            vmem(5, FULL),
            vmem(5, FULL),
            vmem(5, FULL),
            vmem(5, FULL),
            vmem(5, FULL),
            vmem(4, FULL, 2),
            vmem(4, FULL, 2),
            pltpu.SemaphoreType.DMA((4,)),
            pltpu.SemaphoreType.DMA((12,)),
            pltpu.SemaphoreType.DMA((12,)),
            pltpu.SemaphoreType.REGULAR((4,)),
        ],
        compiler_params=pltpu.CompilerParams(
            collective_id=0, has_side_effects=True, vmem_limit_bytes=16 * 1024 * 1024
        ),
        name="force",
    )(pltpu.with_memory_space_constraint(links.reshape(shape), pltpu.HBM))
    return out.reshape(links.shape)


def solution(mesh):
    return jax.shard_map(
        per_device,
        mesh=mesh,
        in_specs=(P(None, None, None, None, "ta", "gz", "gx"),),
        out_specs=P(None, None, None, None, "ta", "gz", "gx"),
        check_vma=False,
    )
```

```python
import jax
import jax.numpy as jnp
from jax import lax
from jax.experimental import pallas as pl
from jax.experimental.pallas import tpu as pltpu
from jax.sharding import PartitionSpec as P

COEFF = -1.9
MESH = pl.DeviceIdType.MESH
AXES = ("ta", "gz", "gx")
ROWS2 = 12
FULL = 18
CORNERS = ((0, 1), (0, 2), (1, 0), (1, 2), (2, 0), (2, 1))


def rs(v, k):
    k = k % 8
    return v if k == 0 else pltpu.roll(v, k, axis=0)


def rl(v, k):
    k = k % 128
    return v if k == 0 else pltpu.roll(v, k, axis=1)


def sublane():
    return lax.broadcasted_iota(jnp.int32, (8, 128), 0)


def lanes():
    return lax.broadcasted_iota(jnp.int32, (8, 128), 1)


def pick(v, index):
    return jnp.take_along_axis(v, index, axis=1, mode="promise_in_bounds")


def total(terms):
    out = terms[0]
    for t in terms[1:]:
        out = out + t
    return out


def mul_nn(a, b):
    return [
        [
            (
                total([a[i][k][0] * b[k][j][0] for k in range(3)])
                - total([a[i][k][1] * b[k][j][1] for k in range(3)]),
                total([a[i][k][0] * b[k][j][1] for k in range(3)])
                + total([a[i][k][1] * b[k][j][0] for k in range(3)]),
            )
            for j in range(3)
        ]
        for i in range(3)
    ]


def mul_hn(a, b):
    return [
        [
            (
                total([a[k][i][0] * b[k][j][0] for k in range(3)])
                + total([a[k][i][1] * b[k][j][1] for k in range(3)]),
                total([a[k][i][0] * b[k][j][1] for k in range(3)])
                - total([a[k][i][1] * b[k][j][0] for k in range(3)]),
            )
            for j in range(3)
        ]
        for i in range(3)
    ]


def mul_nh(a, b):
    return [
        [
            (
                total([a[i][k][0] * b[j][k][0] for k in range(3)])
                + total([a[i][k][1] * b[j][k][1] for k in range(3)]),
                total([a[i][k][1] * b[j][k][0] for k in range(3)])
                - total([a[i][k][0] * b[j][k][1] for k in range(3)]),
            )
            for j in range(3)
        ]
        for i in range(3)
    ]


def third_row(m):
    row = []
    for col in range(3):
        n, q = (col + 1) % 3, (col + 2) % 3
        r0n, i0n = m[0][n]
        r0q, i0q = m[0][q]
        r1n, i1n = m[1][n]
        r1q, i1q = m[1][q]
        row.append(
            (
                (r0n * r1q - i0n * i1q) - (r0q * r1n - i0q * i1n),
                (r0q * i1n + i0q * r1n) - (r0n * i1q + i0n * r1q),
            )
        )
    return row


def anti(w):
    nine = [w[i][i][1] + w[i][i][1] for i in range(3)]
    for i in range(3):
        for j in range(i + 1, 3):
            nine += [w[i][j][0] - w[j][i][0], w[i][j][1] + w[j][i][1]]
    return nine


def gather(entry, rows=3):
    return [[(entry(i * 6 + j), entry(i * 6 + 3 + j)) for j in range(3)] for i in range(rows)]


def scatter(put, m, first=0):
    for i, row in enumerate(m):
        for j, (re, im) in enumerate(row):
            put((first + i) * 6 + j, re)
            put((first + i) * 6 + 3 + j, im)


def kernel(
    x_hbm, o, u, v, p, l, a,
    sf, sb, sc, hf, hb, hc, far, near, lh, own, pf, lf, staple,
    in_sem, send_sem, recv_sem, ready,
):
    me = {axis: lax.axis_index(axis) for axis in AXES}
    size = {axis: lax.axis_size(axis) for axis in AXES}
    beside = {
        (d, step): lax.rem(me[AXES[d]] + (step + size[AXES[d]]), size[AXES[d]])
        for d in range(3)
        for step in (-1, 1)
    }

    def at(*steps):
        return {AXES[d]: beside[d, step] for d, step in steps}

    barrier = pltpu.get_barrier_semaphore()
    targets = [at((d, step)) for d in range(3) for step in (-1, 1)]
    loads = [pltpu.make_async_copy(x_hbm.at[d], u.at[d], in_sem.at[d]) for d in range(4)]
    for load in loads:
        load.start()
    for target in targets:
        pl.semaphore_signal(barrier, inc=1, device_id=target, device_id_type=MESH)
    for load in loads:
        load.wait()

    def link(d, c, h):
        return u[d, (c // 3) % 2, c // 6, c % 3, h]

    sub, lane = sublane(), lanes()
    low = sub < 4
    zrow = lax.rem(sub, 4)
    group = lax.div(lane, 16)
    slot = lax.rem(group, 4)
    xcol = lax.rem(lane, 16)
    row16 = lane - xcol
    to_next = row16 + lax.rem(xcol + 1, 16)
    to_last = row16 + lax.rem(xcol + 15, 16)
    own_row = lax.div(lane, 64) * 64 + 32 + xcol
    next_x = lax.rem(row16 + 112, 128) + lax.rem(xcol + 1, 16)
    time_row = lax.rem(lane + jnp.where(low, 32, 96), 128)

    def pack_tz(c):
        for pair in range(2):
            even, odd = 2 * pair, 2 * pair + 1
            sb[pair, c] = jnp.where(low, rs(link(even, c, 1), 4), link(odd, c, 1))
            if c < ROWS2:
                sf[pair, c] = jnp.where(low, link(even, c, 0), rs(link(odd, c, 0), 4))
        for h in range(2):
            last = rs(link(0, c, h), -3)
            for k in range(1, 4):
                last = jnp.where(zrow == k, rs(link(k, c, h), k - 3), last)
            sb[2 + h, c] = last
            if c < ROWS2:
                first = link(0, c, h)
                for k in range(1, 4):
                    first = jnp.where(zrow == k, rs(link(k, c, h), k), first)
                sf[2 + h, c] = first

    def pack_y(c):
        last = rl(link(0, c, 0), -112)
        for g in range(1, 8):
            last = jnp.where(group == g, rl(link(g % 4, c, g // 4), 16 * (g - 7)), last)
        sb[4, c] = last
        if c < ROWS2:
            first = link(0, c, 0)
            for g in range(1, 8):
                first = jnp.where(group == g, rl(link(g % 4, c, g // 4), 16 * g), first)
            sf[4, c] = first

    for c in range(ROWS2):
        pack_tz(c)
        pack_y(c)

    def merged(items):
        out = items[0][1]
        for mask, value in items[1:]:
            out = jnp.where(mask, value, out)
        return out

    for w in range(2):
        six = range(6)
        sc[0, w] = merged([(sub == r, rs(link(0, w * 6 + r, 1), r - 4)) for r in six])
        sc[1, w] = merged([(group == g, rl(link(0, w * 6 + g, 1), 16 * g)) for g in six])
        sc[2, w] = merged([(sub == r, rs(link(1, w * 6 + r, 0), r - 3)) for r in six])
        sc[3, w] = merged(
            [
                ((group == g) & (zrow == t), rl(rs(link(1, t * 6 + g, w), t - 3), 16 * g))
                for t in range(2)
                for g in six
            ]
        )
        sc[4, w] = merged([(group == g, rl(link(2, w * 6 + g, 0), 16 * (g - 7))) for g in six])
        sc[5, w] = merged(
            [
                ((group == g) & (zrow == t), rl(rs(link(2, t * 6 + g, w), t), 16 * (g - 7)))
                for t in range(2)
                for g in six
            ]
        )

    def send(n, src, dst, target):
        return pltpu.make_async_remote_copy(
            src_ref=src,
            dst_ref=dst,
            send_sem=send_sem.at[n],
            recv_sem=recv_sem.at[n],
            device_id=target,
            device_id_type=MESH,
        )

    corner = [
        send(6 + n, sc.at[n], hc.at[n], at((back, 1), (ahead, -1)))
        for n, (back, ahead) in enumerate(CORNERS)
    ]
    tiles = (pl.ds(0, 2), pl.ds(2, 2), pl.ds(4, 1))
    two = pl.ds(0, ROWS2)
    ahead_faces = [
        send(d, sf.at[tiles[d]], hf.at[tiles[d], two], at((d, -1))) for d in range(3)
    ]
    back_faces = [
        send(3 + d, sb.at[tiles[d], two], hb.at[tiles[d], two], at((d, 1))) for d in range(3)
    ]
    pl.semaphore_wait(barrier, len(targets))
    words = ((0, -1), (0, 1), (2, -1), (2, 1))
    for n, word in enumerate(words):
        pl.semaphore_signal(ready.at[n], inc=1, device_id=at(word), device_id_type=MESH)
    for d in (1, 0, 2):
        back_faces[d].start()
        ahead_faces[d].start()
    for n, through in enumerate(((0,), (2,), (4, 5), (1, 3))):
        pl.semaphore_wait(ready.at[n], 1)
        for m in through:
            corner[m].start()
    for c in range(ROWS2, FULL):
        pack_tz(c)
        pack_y(c)

    def ahead_x(field):
        return pick(field, to_next)

    def products(n, carry):
        pair, h = lax.div(n, 2), lax.rem(n, 2)
        mu = lax.div(pair, 3)
        nu = lax.rem(mu + 1 + lax.rem(pair, 3), 4)
        prod = mul_nn(gather(lambda c: link(mu, c, h)), gather(lambda c: v[pair, c, h]))

        def put_p(c, value):
            p[pair, c, h] = value

        def put_l(c, value):
            l[pair, c, h] = value

        scatter(put_p, prod)
        scatter(put_l, mul_hn(prod, gather(lambda c: link(nu, c, h))))
        return carry

    def plaquettes(n, carry):
        index, h = lax.div(n, 2), lax.rem(n, 2)
        step, mu = lax.div(index, 4), lax.rem(index, 4)
        nu = lax.rem(mu + 1 + step, 4)
        q = mul_nh(
            gather(lambda c: p[mu * 3 + step, c, h]), gather(lambda c: p[nu * 3 + 2 - step, c, h])
        )
        for n, value in enumerate(anti(q)):
            a[index, n, h] = value
        return carry

    def complete(ref, k):
        m = gather(lambda c: ref[k, c], 2)

        def put(c, value):
            ref[k, c] = value

        scatter(put, [third_row(m)], 2)

    def last_products(k, carry):
        prod = mul_nn(gather(lambda c: own[k, c]), gather(lambda c: hf[k, c]))

        def put_p(c, value):
            pf[k, c] = value

        def put_l(c, value):
            lf[k, c] = value

        scatter(put_p, prod)
        scatter(put_l, mul_hn(prod, gather(lambda c: sb[k, c])))
        return carry

    def spread_z(field):
        return jnp.where(
            zrow == 0,
            rs(field, -1),
            jnp.where(zrow == 2, rs(field, 1), jnp.where(zrow == 3, rs(field, 2), field)),
        )

    for c in range(FULL):
        for j in range(3):
            v[j, c, 0] = jnp.where(low, rs(link(1 + j, c, 0), 4), rs(link(1 + j, c, 1), 4))
            for h in range(2):
                v[3 + j, c, h] = rs(link((2 + j) % 4, c, h), -1)
                v[6 + j, c, h] = rl(link((3 + j) % 4, c, h), -16)
                v[9 + j, c, h] = ahead_x(link(j, c, h))
        for h in range(2):
            own[2 + h, c] = spread_z(sb[2 + h, c])
        own[4, c] = pick(sb[4, c], own_row)
    lax.fori_loop(6, 24, products, 0)
    lax.fori_loop(0, 3, lambda j, carry: products(2 * j, carry), 0)
    for c in range(FULL):
        v[2, c, 0] = pick(l[2, c, 0], to_last)
        v[1, c, 0] = rl(l[1, c, 0], 16)
        for h in range(2):
            v[4, c, h] = pick(l[4, c, h], to_last)
            v[6, c, h] = pick(l[6, c, h], to_last)
            v[11, c, h] = rl(l[11, c, h], 16)

    ahead_faces[2].wait_recv()
    complete(hf, 4)
    lax.fori_loop(4, 5, last_products, 0)
    for c in range(FULL):
        for j in range(3):
            nu = (3 + j) % 4
            for h in range(2):
                turn = 16 * (7 - h * 4 - nu)
                p[6 + j, c, h] = jnp.where(group == 7, rl(pf[4, c], turn), p[6 + j, c, h])
                if j == 0:
                    moved = pick(lf[4, c], 16 * (h * 4 + nu) + lax.rem(xcol + 15, 16))
                    v[6, c, h] = jnp.where(group == 7, moved, v[6, c, h])
                else:
                    l[6 + j, c, h] = jnp.where(group == 7, rl(lf[4, c], turn), l[6 + j, c, h])

    ahead_faces[0].wait_recv()
    for k in range(2):
        complete(hf, k)
    for c in range(FULL):
        for j in range(3):
            nu = 1 + j
            halo = hf[nu // 2, c]
            v[j, c, 1] = jnp.where(
                low, rs(link(nu, c, 1), 4), halo if nu % 2 else rs(halo, 4)
            )
    lax.fori_loop(0, 3, lambda j, carry: products(2 * j + 1, carry), 0)
    for c in range(FULL):
        v[2, c, 1] = pick(l[2, c, 1], to_last)
        v[1, c, 1] = rl(l[1, c, 1], 16)
    lax.fori_loop(4, 10, plaquettes, 0)

    ahead_faces[1].wait_recv()
    for k in range(2, 4):
        complete(hf, k)
    lax.fori_loop(2, 4, last_products, 0)
    for c in range(FULL):
        for j in range(3):
            nu = (2 + j) % 4
            for h in range(2):
                p[3 + j, c, h] = jnp.where(zrow == 3, rs(pf[2 + h, c], 3 - nu), p[3 + j, c, h])
                if j == 1:
                    v[4, c, h] = jnp.where(zrow == 3, pick(lf[2 + h, c], to_last), v[4, c, h])
                else:
                    l[3 + j, c, h] = jnp.where(
                        zrow == 3, rs(lf[2 + h, c], 3 - nu), l[3 + j, c, h]
                    )
    lax.fori_loop(0, 4, plaquettes, 0)
    lax.fori_loop(10, 12, plaquettes, 0)

    for c in range(FULL):
        for mu in range(4):
            for h in range(2):
                terms = []
                if mu != 3:
                    terms.append(v[mu * 3 + 2 - mu, c, h])
                if mu != 0:
                    pair = mu * 3 + 3 - mu
                    turned = rs(l[pair, c, 0], 4)
                    if h == 0:
                        terms.append(jnp.where(low, 0.0, turned))
                    else:
                        terms.append(jnp.where(low, turned, rs(l[pair, c, 1], 4)))
                if mu != 1:
                    pair = mu * 3 + (0 - mu) % 4
                    terms.append(jnp.where(zrow == 0, 0.0, rs(l[pair, c, h], 1)))
                if mu != 2:
                    pair = mu * 3 + (1 - mu) % 4
                    moved = rl(l[pair, c, h], 16) if mu == 1 else v[pair, c, h]
                    terms.append(jnp.where(group == 0, 0.0, moved))
                staple[mu, c, h] = total(terms)

    for copy in (back_faces[2], back_faces[0], back_faces[1]):
        copy.wait_recv()
    for k in range(5):
        complete(hb, k)
    for c in range(FULL):
        field = hb[0, c]
        both = jnp.where(low, field, rs(field, 4))
        near[0, c] = both
        near[1, c] = both
        for h in range(2):
            near[2 + h, c] = spread_z(hb[2 + h, c])
        near[4, c] = pick(hb[4, c], own_row)
    for c in range(ROWS2):
        field = hb[0, c]
        far[0, c] = rs(field, 3)
        far[1, c] = jnp.where(low, rl(field, -16), ahead_x(rs(field, 4)))
        for h in range(2):
            field = hb[2 + h, c]
            along_t = rs(field, 3)
            if h == 0:
                along_t = jnp.where(low, along_t, rs(hb[3, c], 3))
            far[2 + h, c] = jnp.where(
                zrow == 0,
                along_t,
                jnp.where(zrow == 3, ahead_x(rs(field, 2)), rl(rs(field, 1), -16)),
            )
        field = hb[4, c]
        along_t = pick(rs(field, 4), time_row)
        along_z = rl(rs(field, -1), -16)
        along_x = pick(field, next_x)
        far[4, c] = jnp.where(slot == 0, along_t, jnp.where(slot == 3, along_x, along_z))

    for copy in corner:
        copy.wait_recv()

    def edge_t0(c):
        return jnp.where(sub == 7, rs(hc[0, c // 6], 7 - c % 6), far[0, c])

    def edge_t1(c):
        edge = rl(rs(hc[1, c // 6], 4), 16 * (7 - c % 6))
        return jnp.where(low & (group == 7), edge, far[1, c])

    def edge_z(h):
        def edge_of(c):
            edge = rl(rs(hc[3, h], 2 - c // 6), 16 * (7 - c % 6))
            out = jnp.where((group == 7) & (zrow == 2), edge, far[2 + h, c])
            if h == 1:
                out = jnp.where(sub == 4, rs(hc[2, c // 6], 4 - c % 6), out)
            return out

        return edge_of

    def edge_y(c):
        along_t = rs(rl(hc[4, c // 6], 16 * (4 - c % 6)), 4)
        edge0 = rs(rl(hc[5, 0], 16 * (1 - c % 6)), 3 - c // 6)
        edge1 = rs(rl(hc[5, 1], 16 * (5 - c % 6)), 3 - c // 6)
        out = jnp.where((group == 4) & (sub >= 4), along_t, far[4, c])
        out = jnp.where((group == 1) & (zrow == 3), edge0, out)
        return jnp.where((group == 5) & (zrow == 3), edge1, out)

    for k, edge in enumerate((edge_t0, edge_t1, edge_z(0), edge_z(1), edge_y)):
        m = gather(edge, 2)

        def put(c, value):
            far[k, c] = value

        scatter(put, m + [third_row(m)])

    def faces(k, carry):
        prod = mul_nn(gather(lambda c: hb[k, c]), gather(lambda c: far[k, c]))

        def put(c, value):
            lh[k, c] = value

        scatter(put, mul_hn(prod, gather(lambda c: near[k, c])))
        return carry

    lax.fori_loop(0, 5, faces, 0)
    for c in range(FULL):
        for mu in range(4):
            for h in range(2):
                out = staple[mu, c, h]
                if mu != 0 and h == 0:
                    halo = lh[mu // 2, c]
                    out = out + jnp.where(low, rs(halo, 4) if mu % 2 else halo, 0.0)
                if mu != 1:
                    out = out + jnp.where(zrow == 0, rs(lh[2 + h, c], -mu), 0.0)
                if mu != 2:
                    halo = rl(lh[4, c], -16 * (h * 4 + mu))
                    out = out + jnp.where(group == 0, halo, 0.0)
                staple[mu, c, h] = out

    def forces(n, carry):
        mu, h = lax.div(n, 2), lax.rem(n, 2)
        w = anti(mul_nn(gather(lambda c: link(mu, c, h)), gather(lambda c: staple[mu, c, h])))
        prev, other = lax.rem(mu + 3, 4), 4 + lax.rem(mu, 2)
        sign = 1.0 - 2.0 * lax.div(mu, 2).astype(jnp.float32)
        nine = [
            w[k] + (a[mu, k, h] - a[prev, k, h] + sign * a[other, k, h]) for k in range(9)
        ]
        third = (nine[0] + nine[1] + nine[2]) * (1.0 / 3.0)
        k = 3
        for i in range(3):
            o[mu, 0, i, i, h] = jnp.zeros((8, 128), jnp.float32)
            o[mu, 1, i, i, h] = (0.5 * COEFF) * (nine[i] - third)
            for j in range(i + 1, 3):
                re, im = (0.5 * COEFF) * nine[k], (0.5 * COEFF) * nine[k + 1]
                o[mu, 0, i, j, h] = re
                o[mu, 0, j, i, h] = -re
                o[mu, 1, i, j, h] = im
                o[mu, 1, j, i, h] = im
                k += 2
        return carry

    lax.fori_loop(0, 8, forces, 0)
    for copy in ahead_faces + back_faces + corner:
        copy.wait_send()


def per_device(links):
    shape = (4, 2, 3, 3, 2, 8, 128)

    def vmem(*lead):
        return pltpu.VMEM(lead + (8, 128), jnp.float32)

    pairs = vmem(12, FULL, 2)
    out = pl.pallas_call(
        kernel,
        out_shape=jax.ShapeDtypeStruct(shape, jnp.float32),
        in_specs=[pl.BlockSpec(memory_space=pltpu.HBM)],
        out_specs=pl.BlockSpec(memory_space=pltpu.VMEM),
        scratch_shapes=[
            vmem(4, 2, 3, 3, 2),
            pairs,
            pairs,
            pairs,
            vmem(6, 9, 2),
            vmem(5, ROWS2),
            vmem(5, FULL),
            vmem(6, 2),
            vmem(5, FULL),
            vmem(5, FULL),
            vmem(6, 2),
            vmem(5, FULL),
            vmem(5, FULL),
            vmem(5, FULL),
            vmem(5, FULL),
            vmem(5, FULL),
            vmem(5, FULL),
            vmem(4, FULL, 2),
            pltpu.SemaphoreType.DMA((4,)),
            pltpu.SemaphoreType.DMA((12,)),
            pltpu.SemaphoreType.DMA((12,)),
            pltpu.SemaphoreType.REGULAR((4,)),
        ],
        compiler_params=pltpu.CompilerParams(
            collective_id=0, has_side_effects=True, vmem_limit_bytes=16 * 1024 * 1024
        ),
        name="force",
    )(pltpu.with_memory_space_constraint(links.reshape(shape), pltpu.HBM))
    return out.reshape(links.shape)


def solution(mesh):
    return jax.shard_map(
        per_device,
        mesh=mesh,
        in_specs=(P(None, None, None, None, "ta", "gz", "gx"),),
        out_specs=P(None, None, None, None, "ta", "gz", "gx"),
        check_vma=False,
    )
```

```python
import jax
import jax.numpy as jnp
from jax import lax
from jax.experimental import pallas as pl
from jax.experimental.pallas import tpu as pltpu
from jax.sharding import PartitionSpec as P

COEFF = -1.9
MESH = pl.DeviceIdType.MESH
AXES = ("ta", "gz", "gx")
ROWS2 = 12
FULL = 18
CORNERS = ((0, 1), (0, 2), (1, 0), (1, 2), (2, 0), (2, 1))


def rs(v, k):
    k = k % 8
    return v if k == 0 else pltpu.roll(v, k, axis=0)


def rl(v, k):
    k = k % 128
    return v if k == 0 else pltpu.roll(v, k, axis=1)


def sublane():
    return lax.broadcasted_iota(jnp.int32, (8, 128), 0)


def lanes():
    return lax.broadcasted_iota(jnp.int32, (8, 128), 1)


def pick(v, index):
    return jnp.take_along_axis(v, index, axis=1, mode="promise_in_bounds")


def total(terms):
    out = terms[0]
    for t in terms[1:]:
        out = out + t
    return out


def mul_nn(a, b):
    return [
        [
            (
                total([a[i][k][0] * b[k][j][0] for k in range(3)])
                - total([a[i][k][1] * b[k][j][1] for k in range(3)]),
                total([a[i][k][0] * b[k][j][1] for k in range(3)])
                + total([a[i][k][1] * b[k][j][0] for k in range(3)]),
            )
            for j in range(3)
        ]
        for i in range(3)
    ]


def mul_hn(a, b):
    return [
        [
            (
                total([a[k][i][0] * b[k][j][0] for k in range(3)])
                + total([a[k][i][1] * b[k][j][1] for k in range(3)]),
                total([a[k][i][0] * b[k][j][1] for k in range(3)])
                - total([a[k][i][1] * b[k][j][0] for k in range(3)]),
            )
            for j in range(3)
        ]
        for i in range(3)
    ]


def mul_nh(a, b):
    return [
        [
            (
                total([a[i][k][0] * b[j][k][0] for k in range(3)])
                + total([a[i][k][1] * b[j][k][1] for k in range(3)]),
                total([a[i][k][1] * b[j][k][0] for k in range(3)])
                - total([a[i][k][0] * b[j][k][1] for k in range(3)]),
            )
            for j in range(3)
        ]
        for i in range(3)
    ]


def third_row(m):
    row = []
    for col in range(3):
        n, q = (col + 1) % 3, (col + 2) % 3
        r0n, i0n = m[0][n]
        r0q, i0q = m[0][q]
        r1n, i1n = m[1][n]
        r1q, i1q = m[1][q]
        row.append(
            (
                (r0n * r1q - i0n * i1q) - (r0q * r1n - i0q * i1n),
                (r0q * i1n + i0q * r1n) - (r0n * i1q + i0n * r1q),
            )
        )
    return row


def anti(w):
    nine = [w[i][i][1] + w[i][i][1] for i in range(3)]
    for i in range(3):
        for j in range(i + 1, 3):
            nine += [w[i][j][0] - w[j][i][0], w[i][j][1] + w[j][i][1]]
    return nine


def gather(entry, rows=3):
    return [[(entry(i * 6 + j), entry(i * 6 + 3 + j)) for j in range(3)] for i in range(rows)]


def scatter(put, m, first=0):
    for i, row in enumerate(m):
        for j, (re, im) in enumerate(row):
            put((first + i) * 6 + j, re)
            put((first + i) * 6 + 3 + j, im)


def kernel(
    x_hbm, o, u, v, p, l, a,
    sf, sb, sc, hf, hb, hc, far, near, lh, own, pf, lf, staple,
    in_sem, send_sem, recv_sem, ready,
):
    me = {axis: lax.axis_index(axis) for axis in AXES}
    size = {axis: lax.axis_size(axis) for axis in AXES}
    beside = {
        (d, step): lax.rem(me[AXES[d]] + (step + size[AXES[d]]), size[AXES[d]])
        for d in range(3)
        for step in (-1, 1)
    }

    def at(*steps):
        return {AXES[d]: beside[d, step] for d, step in steps}

    barrier = pltpu.get_barrier_semaphore()
    targets = [at((d, step)) for d in range(3) for step in (-1, 1)]
    loads = [pltpu.make_async_copy(x_hbm.at[d], u.at[d], in_sem.at[d]) for d in range(4)]
    for load in loads:
        load.start()
    for target in targets:
        pl.semaphore_signal(barrier, inc=1, device_id=target, device_id_type=MESH)
    for load in loads:
        load.wait()

    def link(d, c, h):
        return u[d, (c // 3) % 2, c // 6, c % 3, h]

    sub, lane = sublane(), lanes()
    low = sub < 4
    zrow = lax.rem(sub, 4)
    group = lax.div(lane, 16)
    slot = lax.rem(group, 4)
    xcol = lax.rem(lane, 16)
    row16 = lane - xcol
    to_next = row16 + lax.rem(xcol + 1, 16)
    to_last = row16 + lax.rem(xcol + 15, 16)
    own_row = lax.div(lane, 64) * 64 + 32 + xcol
    next_x = lax.rem(row16 + 112, 128) + lax.rem(xcol + 1, 16)
    time_row = lax.rem(lane + jnp.where(low, 32, 96), 128)

    def pack_tz(c):
        for pair in range(2):
            even, odd = 2 * pair, 2 * pair + 1
            sb[pair, c] = jnp.where(low, rs(link(even, c, 1), 4), link(odd, c, 1))
            if c < ROWS2:
                sf[pair, c] = jnp.where(low, link(even, c, 0), rs(link(odd, c, 0), 4))
        for h in range(2):
            last = rs(link(0, c, h), -3)
            for k in range(1, 4):
                last = jnp.where(zrow == k, rs(link(k, c, h), k - 3), last)
            sb[2 + h, c] = last
            if c < ROWS2:
                first = link(0, c, h)
                for k in range(1, 4):
                    first = jnp.where(zrow == k, rs(link(k, c, h), k), first)
                sf[2 + h, c] = first

    def pack_y(c):
        last = rl(link(0, c, 0), -112)
        for g in range(1, 8):
            last = jnp.where(group == g, rl(link(g % 4, c, g // 4), 16 * (g - 7)), last)
        sb[4, c] = last
        if c < ROWS2:
            first = link(0, c, 0)
            for g in range(1, 8):
                first = jnp.where(group == g, rl(link(g % 4, c, g // 4), 16 * g), first)
            sf[4, c] = first

    for c in range(ROWS2):
        pack_tz(c)
        pack_y(c)

    def merged(items):
        out = items[0][1]
        for mask, value in items[1:]:
            out = jnp.where(mask, value, out)
        return out

    for w in range(2):
        six = range(6)
        sc[0, w] = merged([(sub == r, rs(link(0, w * 6 + r, 1), r - 4)) for r in six])
        sc[1, w] = merged([(group == g, rl(link(0, w * 6 + g, 1), 16 * g)) for g in six])
        sc[2, w] = merged([(sub == r, rs(link(1, w * 6 + r, 0), r - 3)) for r in six])
        sc[3, w] = merged(
            [
                ((group == g) & (zrow == t), rl(rs(link(1, t * 6 + g, w), t - 3), 16 * g))
                for t in range(2)
                for g in six
            ]
        )
        sc[4, w] = merged([(group == g, rl(link(2, w * 6 + g, 0), 16 * (g - 7))) for g in six])
        sc[5, w] = merged(
            [
                ((group == g) & (zrow == t), rl(rs(link(2, t * 6 + g, w), t), 16 * (g - 7)))
                for t in range(2)
                for g in six
            ]
        )

    def send(n, src, dst, target):
        return pltpu.make_async_remote_copy(
            src_ref=src,
            dst_ref=dst,
            send_sem=send_sem.at[n],
            recv_sem=recv_sem.at[n],
            device_id=target,
            device_id_type=MESH,
        )

    corner = [
        send(6 + n, sc.at[n], hc.at[n], at((back, 1), (ahead, -1)))
        for n, (back, ahead) in enumerate(CORNERS)
    ]
    tiles = (pl.ds(0, 2), pl.ds(2, 2), pl.ds(4, 1))
    two = pl.ds(0, ROWS2)
    ahead_faces = [
        send(d, sf.at[tiles[d]], hf.at[tiles[d], two], at((d, -1))) for d in range(3)
    ]
    back_faces = [
        send(3 + d, sb.at[tiles[d], two], hb.at[tiles[d], two], at((d, 1))) for d in range(3)
    ]
    pl.semaphore_wait(barrier, len(targets))
    words = ((0, -1), (0, 1), (1, -1), (1, 1))
    for n, word in enumerate(words):
        pl.semaphore_signal(ready.at[n], inc=1, device_id=at(word), device_id_type=MESH)
    for d in (1, 0, 2):
        back_faces[d].start()
        ahead_faces[d].start()
    for n, through in enumerate(((0, 1), (2, 4), (3,), (5,))):
        pl.semaphore_wait(ready.at[n], 1)
        for m in through:
            corner[m].start()
    for c in range(ROWS2, FULL):
        pack_tz(c)
        pack_y(c)

    def ahead_x(field):
        return pick(field, to_next)

    def products(n, carry):
        pair, h = lax.div(n, 2), lax.rem(n, 2)
        mu = lax.div(pair, 3)
        nu = lax.rem(mu + 1 + lax.rem(pair, 3), 4)
        prod = mul_nn(gather(lambda c: link(mu, c, h)), gather(lambda c: v[pair, c, h]))

        def put_p(c, value):
            p[pair, c, h] = value

        def put_l(c, value):
            l[pair, c, h] = value

        scatter(put_p, prod)
        scatter(put_l, mul_hn(prod, gather(lambda c: link(nu, c, h))))
        return carry

    def plaquettes(n, carry):
        index, h = lax.div(n, 2), lax.rem(n, 2)
        step, mu = lax.div(index, 4), lax.rem(index, 4)
        nu = lax.rem(mu + 1 + step, 4)
        q = mul_nh(
            gather(lambda c: p[mu * 3 + step, c, h]), gather(lambda c: p[nu * 3 + 2 - step, c, h])
        )
        for n, value in enumerate(anti(q)):
            a[index, n, h] = value
        return carry

    def complete(ref, k):
        m = gather(lambda c: ref[k, c], 2)

        def put(c, value):
            ref[k, c] = value

        scatter(put, [third_row(m)], 2)

    def last_products(k, carry):
        prod = mul_nn(gather(lambda c: own[k, c]), gather(lambda c: hf[k, c]))

        def put_p(c, value):
            pf[k, c] = value

        def put_l(c, value):
            lf[k, c] = value

        scatter(put_p, prod)
        scatter(put_l, mul_hn(prod, gather(lambda c: sb[k, c])))
        return carry

    def spread_z(field):
        return jnp.where(
            zrow == 0,
            rs(field, -1),
            jnp.where(zrow == 2, rs(field, 1), jnp.where(zrow == 3, rs(field, 2), field)),
        )

    for c in range(FULL):
        for j in range(3):
            v[j, c, 0] = jnp.where(low, rs(link(1 + j, c, 0), 4), rs(link(1 + j, c, 1), 4))
            for h in range(2):
                v[3 + j, c, h] = rs(link((2 + j) % 4, c, h), -1)
                v[6 + j, c, h] = rl(link((3 + j) % 4, c, h), -16)
                v[9 + j, c, h] = ahead_x(link(j, c, h))
        for h in range(2):
            own[2 + h, c] = spread_z(sb[2 + h, c])
        own[4, c] = pick(sb[4, c], own_row)
    lax.fori_loop(6, 24, products, 0)
    lax.fori_loop(0, 3, lambda j, carry: products(2 * j, carry), 0)
    for c in range(FULL):
        v[2, c, 0] = pick(l[2, c, 0], to_last)
        v[1, c, 0] = rl(l[1, c, 0], 16)
        for h in range(2):
            v[4, c, h] = pick(l[4, c, h], to_last)
            v[6, c, h] = pick(l[6, c, h], to_last)
            v[11, c, h] = rl(l[11, c, h], 16)

    ahead_faces[2].wait_recv()
    complete(hf, 4)
    lax.fori_loop(4, 5, last_products, 0)
    for c in range(FULL):
        for j in range(3):
            nu = (3 + j) % 4
            for h in range(2):
                turn = 16 * (7 - h * 4 - nu)
                p[6 + j, c, h] = jnp.where(group == 7, rl(pf[4, c], turn), p[6 + j, c, h])
                if j == 0:
                    moved = pick(lf[4, c], 16 * (h * 4 + nu) + lax.rem(xcol + 15, 16))
                    v[6, c, h] = jnp.where(group == 7, moved, v[6, c, h])
                else:
                    l[6 + j, c, h] = jnp.where(group == 7, rl(lf[4, c], turn), l[6 + j, c, h])

    ahead_faces[0].wait_recv()
    for k in range(2):
        complete(hf, k)
    for c in range(FULL):
        for j in range(3):
            nu = 1 + j
            halo = hf[nu // 2, c]
            v[j, c, 1] = jnp.where(
                low, rs(link(nu, c, 1), 4), halo if nu % 2 else rs(halo, 4)
            )
    lax.fori_loop(0, 3, lambda j, carry: products(2 * j + 1, carry), 0, unroll=3)
    for c in range(FULL):
        v[2, c, 1] = pick(l[2, c, 1], to_last)
        v[1, c, 1] = rl(l[1, c, 1], 16)
    lax.fori_loop(4, 10, plaquettes, 0, unroll=2)

    ahead_faces[1].wait_recv()
    for k in range(2, 4):
        complete(hf, k)
    lax.fori_loop(2, 4, last_products, 0, unroll=2)
    for c in range(FULL):
        for j in range(3):
            nu = (2 + j) % 4
            for h in range(2):
                p[3 + j, c, h] = jnp.where(zrow == 3, rs(pf[2 + h, c], 3 - nu), p[3 + j, c, h])
                if j == 1:
                    v[4, c, h] = jnp.where(zrow == 3, pick(lf[2 + h, c], to_last), v[4, c, h])
                else:
                    l[3 + j, c, h] = jnp.where(
                        zrow == 3, rs(lf[2 + h, c], 3 - nu), l[3 + j, c, h]
                    )
    lax.fori_loop(0, 4, plaquettes, 0, unroll=2)
    lax.fori_loop(10, 12, plaquettes, 0, unroll=2)

    for c in range(FULL):
        for mu in range(4):
            for h in range(2):
                terms = []
                if mu != 3:
                    terms.append(v[mu * 3 + 2 - mu, c, h])
                if mu != 0:
                    pair = mu * 3 + 3 - mu
                    turned = rs(l[pair, c, 0], 4)
                    if h == 0:
                        terms.append(jnp.where(low, 0.0, turned))
                    else:
                        terms.append(jnp.where(low, turned, rs(l[pair, c, 1], 4)))
                if mu != 1:
                    pair = mu * 3 + (0 - mu) % 4
                    terms.append(jnp.where(zrow == 0, 0.0, rs(l[pair, c, h], 1)))
                if mu != 2:
                    pair = mu * 3 + (1 - mu) % 4
                    moved = rl(l[pair, c, h], 16) if mu == 1 else v[pair, c, h]
                    terms.append(jnp.where(group == 0, 0.0, moved))
                staple[mu, c, h] = total(terms)

    for copy in (back_faces[2], back_faces[0], back_faces[1]):
        copy.wait_recv()
    for k in range(5):
        complete(hb, k)
    for c in range(FULL):
        field = hb[0, c]
        both = jnp.where(low, field, rs(field, 4))
        near[0, c] = both
        near[1, c] = both
        for h in range(2):
            near[2 + h, c] = spread_z(hb[2 + h, c])
        near[4, c] = pick(hb[4, c], own_row)
    for c in range(ROWS2):
        field = hb[0, c]
        far[0, c] = rs(field, 3)
        far[1, c] = jnp.where(low, rl(field, -16), ahead_x(rs(field, 4)))
        for h in range(2):
            field = hb[2 + h, c]
            along_t = rs(field, 3)
            if h == 0:
                along_t = jnp.where(low, along_t, rs(hb[3, c], 3))
            far[2 + h, c] = jnp.where(
                zrow == 0,
                along_t,
                jnp.where(zrow == 3, ahead_x(rs(field, 2)), rl(rs(field, 1), -16)),
            )
        field = hb[4, c]
        along_t = pick(rs(field, 4), time_row)
        along_z = rl(rs(field, -1), -16)
        along_x = pick(field, next_x)
        far[4, c] = jnp.where(slot == 0, along_t, jnp.where(slot == 3, along_x, along_z))

    for copy in corner:
        copy.wait_recv()

    def edge_t0(c):
        return jnp.where(sub == 7, rs(hc[0, c // 6], 7 - c % 6), far[0, c])

    def edge_t1(c):
        edge = rl(rs(hc[1, c // 6], 4), 16 * (7 - c % 6))
        return jnp.where(low & (group == 7), edge, far[1, c])

    def edge_z(h):
        def edge_of(c):
            edge = rl(rs(hc[3, h], 2 - c // 6), 16 * (7 - c % 6))
            out = jnp.where((group == 7) & (zrow == 2), edge, far[2 + h, c])
            if h == 1:
                out = jnp.where(sub == 4, rs(hc[2, c // 6], 4 - c % 6), out)
            return out

        return edge_of

    def edge_y(c):
        along_t = rs(rl(hc[4, c // 6], 16 * (4 - c % 6)), 4)
        edge0 = rs(rl(hc[5, 0], 16 * (1 - c % 6)), 3 - c // 6)
        edge1 = rs(rl(hc[5, 1], 16 * (5 - c % 6)), 3 - c // 6)
        out = jnp.where((group == 4) & (sub >= 4), along_t, far[4, c])
        out = jnp.where((group == 1) & (zrow == 3), edge0, out)
        return jnp.where((group == 5) & (zrow == 3), edge1, out)

    for k, edge in enumerate((edge_t0, edge_t1, edge_z(0), edge_z(1), edge_y)):
        m = gather(edge, 2)

        def put(c, value):
            far[k, c] = value

        scatter(put, m + [third_row(m)])

    def faces(k, carry):
        prod = mul_nn(gather(lambda c: hb[k, c]), gather(lambda c: far[k, c]))

        def put(c, value):
            lh[k, c] = value

        scatter(put, mul_hn(prod, gather(lambda c: near[k, c])))
        return carry

    lax.fori_loop(0, 5, faces, 0, unroll=5)
    for c in range(FULL):
        for mu in range(4):
            for h in range(2):
                out = staple[mu, c, h]
                if mu != 0 and h == 0:
                    halo = lh[mu // 2, c]
                    out = out + jnp.where(low, rs(halo, 4) if mu % 2 else halo, 0.0)
                if mu != 1:
                    out = out + jnp.where(zrow == 0, rs(lh[2 + h, c], -mu), 0.0)
                if mu != 2:
                    halo = rl(lh[4, c], -16 * (h * 4 + mu))
                    out = out + jnp.where(group == 0, halo, 0.0)
                staple[mu, c, h] = out

    def forces(n, carry):
        mu, h = lax.div(n, 2), lax.rem(n, 2)
        w = anti(mul_nn(gather(lambda c: link(mu, c, h)), gather(lambda c: staple[mu, c, h])))
        prev, other = lax.rem(mu + 3, 4), 4 + lax.rem(mu, 2)
        sign = 1.0 - 2.0 * lax.div(mu, 2).astype(jnp.float32)
        nine = [
            w[k] + (a[mu, k, h] - a[prev, k, h] + sign * a[other, k, h]) for k in range(9)
        ]
        third = (nine[0] + nine[1] + nine[2]) * (1.0 / 3.0)
        k = 3
        for i in range(3):
            o[mu, 0, i, i, h] = jnp.zeros((8, 128), jnp.float32)
            o[mu, 1, i, i, h] = (0.5 * COEFF) * (nine[i] - third)
            for j in range(i + 1, 3):
                re, im = (0.5 * COEFF) * nine[k], (0.5 * COEFF) * nine[k + 1]
                o[mu, 0, i, j, h] = re
                o[mu, 0, j, i, h] = -re
                o[mu, 1, i, j, h] = im
                o[mu, 1, j, i, h] = im
                k += 2
        return carry

    lax.fori_loop(0, 8, forces, 0, unroll=4)
    for copy in ahead_faces + back_faces + corner:
        copy.wait_send()


def per_device(links):
    shape = (4, 2, 3, 3, 2, 8, 128)

    def vmem(*lead):
        return pltpu.VMEM(lead + (8, 128), jnp.float32)

    pairs = vmem(12, FULL, 2)
    out = pl.pallas_call(
        kernel,
        out_shape=jax.ShapeDtypeStruct(shape, jnp.float32),
        in_specs=[pl.BlockSpec(memory_space=pltpu.HBM)],
        out_specs=pl.BlockSpec(memory_space=pltpu.VMEM),
        scratch_shapes=[
            vmem(4, 2, 3, 3, 2),
            pairs,
            pairs,
            pairs,
            vmem(6, 9, 2),
            vmem(5, ROWS2),
            vmem(5, FULL),
            vmem(6, 2),
            vmem(5, FULL),
            vmem(5, FULL),
            vmem(6, 2),
            vmem(5, FULL),
            vmem(5, FULL),
            vmem(5, FULL),
            vmem(5, FULL),
            vmem(5, FULL),
            vmem(5, FULL),
            vmem(4, FULL, 2),
            pltpu.SemaphoreType.DMA((4,)),
            pltpu.SemaphoreType.DMA((12,)),
            pltpu.SemaphoreType.DMA((12,)),
            pltpu.SemaphoreType.REGULAR((4,)),
        ],
        compiler_params=pltpu.CompilerParams(
            collective_id=0, has_side_effects=True, vmem_limit_bytes=16 * 1024 * 1024
        ),
        name="force",
    )(pltpu.with_memory_space_constraint(links.reshape(shape), pltpu.HBM))
    return out.reshape(links.shape)


def solution(mesh):
    return jax.shard_map(
        per_device,
        mesh=mesh,
        in_specs=(P(None, None, None, None, "ta", "gz", "gx"),),
        out_specs=P(None, None, None, None, "ta", "gz", "gx"),
        check_vma=False,
    )
```

```python
import jax
import jax.numpy as jnp
from jax import lax
from jax.experimental import pallas as pl
from jax.experimental.pallas import tpu as pltpu
from jax.sharding import PartitionSpec as P

COEFF = -1.9
MESH = pl.DeviceIdType.MESH
AXES = ("ta", "gz", "gx")
ROWS2 = 12
FULL = 18
CORNERS = ((0, 1), (0, 2), (1, 0), (1, 2), (2, 0), (2, 1))


def rs(v, k):
    k = k % 8
    return v if k == 0 else pltpu.roll(v, k, axis=0)


def rl(v, k):
    k = k % 128
    return v if k == 0 else pltpu.roll(v, k, axis=1)


def sublane():
    return lax.broadcasted_iota(jnp.int32, (8, 128), 0)


def lanes():
    return lax.broadcasted_iota(jnp.int32, (8, 128), 1)


def pick(v, index):
    return jnp.take_along_axis(v, index, axis=1, mode="promise_in_bounds")


def total(terms):
    out = terms[0]
    for t in terms[1:]:
        out = out + t
    return out


def mul_nn(a, b):
    return [
        [
            (
                total([a[i][k][0] * b[k][j][0] for k in range(3)])
                - total([a[i][k][1] * b[k][j][1] for k in range(3)]),
                total([a[i][k][0] * b[k][j][1] for k in range(3)])
                + total([a[i][k][1] * b[k][j][0] for k in range(3)]),
            )
            for j in range(3)
        ]
        for i in range(3)
    ]


def mul_hn(a, b):
    return [
        [
            (
                total([a[k][i][0] * b[k][j][0] for k in range(3)])
                + total([a[k][i][1] * b[k][j][1] for k in range(3)]),
                total([a[k][i][0] * b[k][j][1] for k in range(3)])
                - total([a[k][i][1] * b[k][j][0] for k in range(3)]),
            )
            for j in range(3)
        ]
        for i in range(3)
    ]


def mul_nh(a, b):
    return [
        [
            (
                total([a[i][k][0] * b[j][k][0] for k in range(3)])
                + total([a[i][k][1] * b[j][k][1] for k in range(3)]),
                total([a[i][k][1] * b[j][k][0] for k in range(3)])
                - total([a[i][k][0] * b[j][k][1] for k in range(3)]),
            )
            for j in range(3)
        ]
        for i in range(3)
    ]


def third_row(m):
    row = []
    for col in range(3):
        n, q = (col + 1) % 3, (col + 2) % 3
        r0n, i0n = m[0][n]
        r0q, i0q = m[0][q]
        r1n, i1n = m[1][n]
        r1q, i1q = m[1][q]
        row.append(
            (
                (r0n * r1q - i0n * i1q) - (r0q * r1n - i0q * i1n),
                (r0q * i1n + i0q * r1n) - (r0n * i1q + i0n * r1q),
            )
        )
    return row


def anti(w):
    nine = [w[i][i][1] + w[i][i][1] for i in range(3)]
    for i in range(3):
        for j in range(i + 1, 3):
            nine += [w[i][j][0] - w[j][i][0], w[i][j][1] + w[j][i][1]]
    return nine


def gather(entry, rows=3):
    return [[(entry(i * 6 + j), entry(i * 6 + 3 + j)) for j in range(3)] for i in range(rows)]


def scatter(put, m, first=0):
    for i, row in enumerate(m):
        for j, (re, im) in enumerate(row):
            put((first + i) * 6 + j, re)
            put((first + i) * 6 + 3 + j, im)


def kernel(
    x_hbm, o, u, v, p, l, a,
    sf, sb, sc, hf, hb, hc, far, near, lh, own, pf, lf, staple,
    in_sem, send_sem, recv_sem, ready,
):
    me = {axis: lax.axis_index(axis) for axis in AXES}
    size = {axis: lax.axis_size(axis) for axis in AXES}
    beside = {
        (d, step): lax.rem(me[AXES[d]] + (step + size[AXES[d]]), size[AXES[d]])
        for d in range(3)
        for step in (-1, 1)
    }

    def at(*steps):
        return {AXES[d]: beside[d, step] for d, step in steps}

    barrier = pltpu.get_barrier_semaphore()
    targets = [at((d, step)) for d in range(3) for step in (-1, 1)]
    loads = [pltpu.make_async_copy(x_hbm.at[d], u.at[d], in_sem.at[d]) for d in range(4)]
    for load in loads:
        load.start()
    for target in targets:
        pl.semaphore_signal(barrier, inc=1, device_id=target, device_id_type=MESH)
    for load in loads:
        load.wait()

    def link(d, c, h):
        return u[d, (c // 3) % 2, c // 6, c % 3, h]

    sub, lane = sublane(), lanes()
    low = sub < 4
    zrow = lax.rem(sub, 4)
    group = lax.div(lane, 16)
    slot = lax.rem(group, 4)
    xcol = lax.rem(lane, 16)
    row16 = lane - xcol
    to_next = row16 + lax.rem(xcol + 1, 16)
    to_last = row16 + lax.rem(xcol + 15, 16)
    own_row = lax.div(lane, 64) * 64 + 32 + xcol
    next_x = lax.rem(row16 + 112, 128) + lax.rem(xcol + 1, 16)
    time_row = lax.rem(lane + jnp.where(low, 32, 96), 128)

    def pack_tz(c):
        for pair in range(2):
            even, odd = 2 * pair, 2 * pair + 1
            sb[pair, c] = jnp.where(low, rs(link(even, c, 1), 4), link(odd, c, 1))
            if c < ROWS2:
                sf[pair, c] = jnp.where(low, link(even, c, 0), rs(link(odd, c, 0), 4))
        for h in range(2):
            last = rs(link(0, c, h), -3)
            for k in range(1, 4):
                last = jnp.where(zrow == k, rs(link(k, c, h), k - 3), last)
            sb[2 + h, c] = last
            if c < ROWS2:
                first = link(0, c, h)
                for k in range(1, 4):
                    first = jnp.where(zrow == k, rs(link(k, c, h), k), first)
                sf[2 + h, c] = first

    def pack_y(c):
        last = rl(link(0, c, 0), -112)
        for g in range(1, 8):
            last = jnp.where(group == g, rl(link(g % 4, c, g // 4), 16 * (g - 7)), last)
        sb[4, c] = last
        if c < ROWS2:
            first = link(0, c, 0)
            for g in range(1, 8):
                first = jnp.where(group == g, rl(link(g % 4, c, g // 4), 16 * g), first)
            sf[4, c] = first

    for c in range(ROWS2):
        pack_tz(c)
        pack_y(c)

    def merged(items):
        out = items[0][1]
        for mask, value in items[1:]:
            out = jnp.where(mask, value, out)
        return out

    for w in range(2):
        six = range(6)
        sc[0, w] = merged([(sub == r, rs(link(0, w * 6 + r, 1), r - 4)) for r in six])
        sc[1, w] = merged([(group == g, rl(link(0, w * 6 + g, 1), 16 * g)) for g in six])
        sc[2, w] = merged([(sub == r, rs(link(1, w * 6 + r, 0), r - 3)) for r in six])
        sc[3, w] = merged(
            [
                ((group == g) & (zrow == t), rl(rs(link(1, t * 6 + g, w), t - 3), 16 * g))
                for t in range(2)
                for g in six
            ]
        )
        sc[4, w] = merged([(group == g, rl(link(2, w * 6 + g, 0), 16 * (g - 7))) for g in six])
        sc[5, w] = merged(
            [
                ((group == g) & (zrow == t), rl(rs(link(2, t * 6 + g, w), t), 16 * (g - 7)))
                for t in range(2)
                for g in six
            ]
        )

    def send(n, src, dst, target):
        return pltpu.make_async_remote_copy(
            src_ref=src,
            dst_ref=dst,
            send_sem=send_sem.at[n],
            recv_sem=recv_sem.at[n],
            device_id=target,
            device_id_type=MESH,
        )

    corner = [
        send(6 + n, sc.at[n], hc.at[n], at((back, 1), (ahead, -1)))
        for n, (back, ahead) in enumerate(CORNERS)
    ]
    tiles = (pl.ds(0, 2), pl.ds(2, 2), pl.ds(4, 1))
    two = pl.ds(0, ROWS2)
    ahead_faces = [
        send(d, sf.at[tiles[d]], hf.at[tiles[d], two], at((d, -1))) for d in range(3)
    ]
    back_faces = [
        send(3 + d, sb.at[tiles[d], two], hb.at[tiles[d], two], at((d, 1))) for d in range(3)
    ]
    pl.semaphore_wait(barrier, len(targets))
    words = ((0, -1), (0, 1), (1, -1), (1, 1))
    for n, word in enumerate(words):
        pl.semaphore_signal(ready.at[n], inc=1, device_id=at(word), device_id_type=MESH)
    for d in (1, 0, 2):
        back_faces[d].start()
        ahead_faces[d].start()
    for n, through in enumerate(((0, 1), (2, 4), (3,), (5,))):
        pl.semaphore_wait(ready.at[n], 1)
        for m in through:
            corner[m].start()
    for c in range(ROWS2, FULL):
        pack_tz(c)
        pack_y(c)

    def ahead_x(field):
        return pick(field, to_next)

    def products(n, carry):
        pair, h = lax.div(n, 2), lax.rem(n, 2)
        mu = lax.div(pair, 3)
        nu = lax.rem(mu + 1 + lax.rem(pair, 3), 4)
        prod = mul_nn(gather(lambda c: link(mu, c, h)), gather(lambda c: v[pair, c, h]))

        def put_p(c, value):
            p[pair, c, h] = value

        def put_l(c, value):
            l[pair, c, h] = value

        scatter(put_p, prod)
        scatter(put_l, mul_hn(prod, gather(lambda c: link(nu, c, h))))
        return carry

    def plaquettes(n, carry):
        index, h = lax.div(n, 2), lax.rem(n, 2)
        step, mu = lax.div(index, 4), lax.rem(index, 4)
        nu = lax.rem(mu + 1 + step, 4)
        q = mul_nh(
            gather(lambda c: p[mu * 3 + step, c, h]), gather(lambda c: p[nu * 3 + 2 - step, c, h])
        )
        for n, value in enumerate(anti(q)):
            a[index, n, h] = value
        return carry

    def complete(ref, k):
        m = gather(lambda c: ref[k, c], 2)

        def put(c, value):
            ref[k, c] = value

        scatter(put, [third_row(m)], 2)

    def last_products(k, carry):
        prod = mul_nn(gather(lambda c: own[k, c]), gather(lambda c: hf[k, c]))

        def put_p(c, value):
            pf[k, c] = value

        def put_l(c, value):
            lf[k, c] = value

        scatter(put_p, prod)
        scatter(put_l, mul_hn(prod, gather(lambda c: sb[k, c])))
        return carry

    def spread_z(field):
        return jnp.where(
            zrow == 0,
            rs(field, -1),
            jnp.where(zrow == 2, rs(field, 1), jnp.where(zrow == 3, rs(field, 2), field)),
        )

    for c in range(FULL):
        for j in range(3):
            v[j, c, 0] = jnp.where(low, rs(link(1 + j, c, 0), 4), rs(link(1 + j, c, 1), 4))
            for h in range(2):
                v[3 + j, c, h] = rs(link((2 + j) % 4, c, h), -1)
                v[6 + j, c, h] = rl(link((3 + j) % 4, c, h), -16)
                v[9 + j, c, h] = ahead_x(link(j, c, h))
        for h in range(2):
            own[2 + h, c] = spread_z(sb[2 + h, c])
        own[4, c] = pick(sb[4, c], own_row)
    lax.fori_loop(6, 24, products, 0)
    lax.fori_loop(0, 3, lambda j, carry: products(2 * j, carry), 0)
    for c in range(FULL):
        v[2, c, 0] = pick(l[2, c, 0], to_last)
        v[1, c, 0] = rl(l[1, c, 0], 16)
        for h in range(2):
            v[4, c, h] = pick(l[4, c, h], to_last)
            v[6, c, h] = pick(l[6, c, h], to_last)
            v[11, c, h] = rl(l[11, c, h], 16)

    def own_staples(mu, c, h):
        terms = []
        if mu != 3:
            terms.append(v[mu * 3 + 2 - mu, c, h])
        if mu != 0:
            pair = mu * 3 + 3 - mu
            turned = rs(l[pair, c, 0], 4)
            if h == 0:
                terms.append(jnp.where(low, 0.0, turned))
            else:
                terms.append(jnp.where(low, turned, rs(l[pair, c, 1], 4)))
        if mu != 1:
            pair = mu * 3 + (0 - mu) % 4
            terms.append(jnp.where(zrow == 0, 0.0, rs(l[pair, c, h], 1)))
        if mu != 2:
            pair = mu * 3 + (1 - mu) % 4
            moved = rl(l[pair, c, h], 16) if mu == 1 else v[pair, c, h]
            terms.append(jnp.where(group == 0, 0.0, moved))
        return total(terms)

    for c in range(FULL):
        staple[0, c, 0] = own_staples(0, c, 0)
        for h in range(2):
            staple[3, c, h] = own_staples(3, c, h)

    ahead_faces[2].wait_recv()
    complete(hf, 4)
    lax.fori_loop(4, 5, last_products, 0)
    for c in range(FULL):
        for j in range(3):
            nu = (3 + j) % 4
            for h in range(2):
                turn = 16 * (7 - h * 4 - nu)
                p[6 + j, c, h] = jnp.where(group == 7, rl(pf[4, c], turn), p[6 + j, c, h])
                if j == 0:
                    moved = pick(lf[4, c], 16 * (h * 4 + nu) + lax.rem(xcol + 15, 16))
                    v[6, c, h] = jnp.where(group == 7, moved, v[6, c, h])
                else:
                    l[6 + j, c, h] = jnp.where(group == 7, rl(lf[4, c], turn), l[6 + j, c, h])

    ahead_faces[0].wait_recv()
    for k in range(2):
        complete(hf, k)
    for c in range(FULL):
        for j in range(3):
            nu = 1 + j
            halo = hf[nu // 2, c]
            v[j, c, 1] = jnp.where(
                low, rs(link(nu, c, 1), 4), halo if nu % 2 else rs(halo, 4)
            )
    lax.fori_loop(0, 3, lambda j, carry: products(2 * j + 1, carry), 0, unroll=3)
    for c in range(FULL):
        v[2, c, 1] = pick(l[2, c, 1], to_last)
        v[1, c, 1] = rl(l[1, c, 1], 16)
    lax.fori_loop(4, 10, plaquettes, 0, unroll=3)

    ahead_faces[1].wait_recv()
    for k in range(2, 4):
        complete(hf, k)
    lax.fori_loop(2, 4, last_products, 0, unroll=2)
    for c in range(FULL):
        for j in range(3):
            nu = (2 + j) % 4
            for h in range(2):
                p[3 + j, c, h] = jnp.where(zrow == 3, rs(pf[2 + h, c], 3 - nu), p[3 + j, c, h])
                if j == 1:
                    v[4, c, h] = jnp.where(zrow == 3, pick(lf[2 + h, c], to_last), v[4, c, h])
                else:
                    l[3 + j, c, h] = jnp.where(
                        zrow == 3, rs(lf[2 + h, c], 3 - nu), l[3 + j, c, h]
                    )
    lax.fori_loop(0, 4, plaquettes, 0, unroll=4)
    lax.fori_loop(10, 12, plaquettes, 0, unroll=2)

    for c in range(FULL):
        for mu in range(3):
            for h in range(0 if mu else 1, 2):
                staple[mu, c, h] = own_staples(mu, c, h)

    for copy in (back_faces[2], back_faces[0], back_faces[1]):
        copy.wait_recv()
    for k in range(5):
        complete(hb, k)
    for c in range(FULL):
        field = hb[0, c]
        both = jnp.where(low, field, rs(field, 4))
        near[0, c] = both
        near[1, c] = both
        for h in range(2):
            near[2 + h, c] = spread_z(hb[2 + h, c])
        near[4, c] = pick(hb[4, c], own_row)
    for c in range(ROWS2):
        field = hb[0, c]
        far[0, c] = rs(field, 3)
        far[1, c] = jnp.where(low, rl(field, -16), ahead_x(rs(field, 4)))
        for h in range(2):
            field = hb[2 + h, c]
            along_t = rs(field, 3)
            if h == 0:
                along_t = jnp.where(low, along_t, rs(hb[3, c], 3))
            far[2 + h, c] = jnp.where(
                zrow == 0,
                along_t,
                jnp.where(zrow == 3, ahead_x(rs(field, 2)), rl(rs(field, 1), -16)),
            )
        field = hb[4, c]
        along_t = pick(rs(field, 4), time_row)
        along_z = rl(rs(field, -1), -16)
        along_x = pick(field, next_x)
        far[4, c] = jnp.where(slot == 0, along_t, jnp.where(slot == 3, along_x, along_z))

    for copy in corner:
        copy.wait_recv()

    def edge_t0(c):
        return jnp.where(sub == 7, rs(hc[0, c // 6], 7 - c % 6), far[0, c])

    def edge_t1(c):
        edge = rl(rs(hc[1, c // 6], 4), 16 * (7 - c % 6))
        return jnp.where(low & (group == 7), edge, far[1, c])

    def edge_z(h):
        def edge_of(c):
            edge = rl(rs(hc[3, h], 2 - c // 6), 16 * (7 - c % 6))
            out = jnp.where((group == 7) & (zrow == 2), edge, far[2 + h, c])
            if h == 1:
                out = jnp.where(sub == 4, rs(hc[2, c // 6], 4 - c % 6), out)
            return out

        return edge_of

    def edge_y(c):
        along_t = rs(rl(hc[4, c // 6], 16 * (4 - c % 6)), 4)
        edge0 = rs(rl(hc[5, 0], 16 * (1 - c % 6)), 3 - c // 6)
        edge1 = rs(rl(hc[5, 1], 16 * (5 - c % 6)), 3 - c // 6)
        out = jnp.where((group == 4) & (sub >= 4), along_t, far[4, c])
        out = jnp.where((group == 1) & (zrow == 3), edge0, out)
        return jnp.where((group == 5) & (zrow == 3), edge1, out)

    for k, edge in enumerate((edge_t0, edge_t1, edge_z(0), edge_z(1), edge_y)):
        m = gather(edge, 2)

        def put(c, value):
            far[k, c] = value

        scatter(put, m + [third_row(m)])

    def faces(k, carry):
        prod = mul_nn(gather(lambda c: hb[k, c]), gather(lambda c: far[k, c]))

        def put(c, value):
            lh[k, c] = value

        scatter(put, mul_hn(prod, gather(lambda c: near[k, c])))
        return carry

    lax.fori_loop(0, 5, faces, 0, unroll=5)
    for c in range(FULL):
        for mu in range(4):
            for h in range(2):
                out = staple[mu, c, h]
                if mu != 0 and h == 0:
                    halo = lh[mu // 2, c]
                    out = out + jnp.where(low, rs(halo, 4) if mu % 2 else halo, 0.0)
                if mu != 1:
                    out = out + jnp.where(zrow == 0, rs(lh[2 + h, c], -mu), 0.0)
                if mu != 2:
                    halo = rl(lh[4, c], -16 * (h * 4 + mu))
                    out = out + jnp.where(group == 0, halo, 0.0)
                staple[mu, c, h] = out

    def forces(n, carry):
        mu, h = lax.div(n, 2), lax.rem(n, 2)
        w = anti(mul_nn(gather(lambda c: link(mu, c, h)), gather(lambda c: staple[mu, c, h])))
        prev, other = lax.rem(mu + 3, 4), 4 + lax.rem(mu, 2)
        sign = 1.0 - 2.0 * lax.div(mu, 2).astype(jnp.float32)
        nine = [
            w[k] + (a[mu, k, h] - a[prev, k, h] + sign * a[other, k, h]) for k in range(9)
        ]
        third = (nine[0] + nine[1] + nine[2]) * (1.0 / 3.0)
        k = 3
        for i in range(3):
            o[mu, 0, i, i, h] = jnp.zeros((8, 128), jnp.float32)
            o[mu, 1, i, i, h] = (0.5 * COEFF) * (nine[i] - third)
            for j in range(i + 1, 3):
                re, im = (0.5 * COEFF) * nine[k], (0.5 * COEFF) * nine[k + 1]
                o[mu, 0, i, j, h] = re
                o[mu, 0, j, i, h] = -re
                o[mu, 1, i, j, h] = im
                o[mu, 1, j, i, h] = im
                k += 2
        return carry

    lax.fori_loop(0, 8, forces, 0, unroll=8)
    for copy in ahead_faces + back_faces + corner:
        copy.wait_send()


def per_device(links):
    shape = (4, 2, 3, 3, 2, 8, 128)

    def vmem(*lead):
        return pltpu.VMEM(lead + (8, 128), jnp.float32)

    pairs = vmem(12, FULL, 2)
    out = pl.pallas_call(
        kernel,
        out_shape=jax.ShapeDtypeStruct(shape, jnp.float32),
        in_specs=[pl.BlockSpec(memory_space=pltpu.HBM)],
        out_specs=pl.BlockSpec(memory_space=pltpu.VMEM),
        scratch_shapes=[
            vmem(4, 2, 3, 3, 2),
            pairs,
            pairs,
            pairs,
            vmem(6, 9, 2),
            vmem(5, ROWS2),
            vmem(5, FULL),
            vmem(6, 2),
            vmem(5, FULL),
            vmem(5, FULL),
            vmem(6, 2),
            vmem(5, FULL),
            vmem(5, FULL),
            vmem(5, FULL),
            vmem(5, FULL),
            vmem(5, FULL),
            vmem(5, FULL),
            vmem(4, FULL, 2),
            pltpu.SemaphoreType.DMA((4,)),
            pltpu.SemaphoreType.DMA((12,)),
            pltpu.SemaphoreType.DMA((12,)),
            pltpu.SemaphoreType.REGULAR((4,)),
        ],
        compiler_params=pltpu.CompilerParams(
            collective_id=0, has_side_effects=True, vmem_limit_bytes=16 * 1024 * 1024
        ),
        name="force",
    )(pltpu.with_memory_space_constraint(links.reshape(shape), pltpu.HBM))
    return out.reshape(links.shape)


def solution(mesh):
    return jax.shard_map(
        per_device,
        mesh=mesh,
        in_specs=(P(None, None, None, None, "ta", "gz", "gx"),),
        out_specs=P(None, None, None, None, "ta", "gz", "gx"),
        check_vma=False,
    )
```
